128 devices in a mesh: gx: 8 (over y, z_hi), gy: 4 (over x), gz: 4 (over z_lo, core).
Axes of the slice: x: 4, y: 4, z: 4 (z_hi: 2, z_lo: 2; z = z_hi * 2 + z_lo), core: 2. Of those that a mesh axis runs over, the one named last changes fastest.
Arguments:
- log_range: float32 [256, 128, 512], P('gx', 'gy', 'gz'), may hold values from 0.7 to 2
- state: float32 [2, 256, 128, 512], P(None, 'gx', 'gy', 'gz'), may hold values from -60 to 60, as said below
- adjoint_start: float32 [2, 256, 128, 512], P(None, 'gx', 'gy', 'gz'), may hold values from -0.3 to 0.3
- obs_index: int32 [2, 8, 4, 4, 4096], P(None, 'gx', 'gy', 'gz'), may hold values from 0 to 131071
- obs_value: float32 [2, 8, 4, 4, 4096], P(None, 'gx', 'gy', 'gz'), may hold values from -6 to 6
Outputs:
- gradient: float32 [256, 128, 512], P('gx', 'gy', 'gz')
- adjoint: float32 [2, 256, 128, 512], P(None, 'gx', 'gy', 'gz')
The draws below stay inside these ranges and needn't reach their ends.
Inputs may be any that keep to these rules, and one draw needn't show every extreme that they name: `obs_index`: each entry numbers a cell of its own device's block as (a * 32 + b) * 128 + c; cells may repeat. `state`: real values.
All inputs are finite; a program needn't handle non-finite values.
Results may differ from the reference program's by a relative error of at most 0.0001.
Values sent between devices are 32-bit elements; how exact they have to be, the bound alone decides.
A program may use at most 320 MiB of HBM per device.

```python
import jax
import jax.numpy as jnp

CX = 32
CY = 32
CZ = 128
NOBS = 4096
REPS = 2
ITERS = 4
NX = 256
NY = 128
NZ = 512
N_GX = 8
N_GY = 4
N_GZ = 4


def draw_state(key, part):
    along_x = (jnp.arange(NX, dtype=jnp.float32) / NX).reshape(-1, 1, 1)
    along_y = (jnp.arange(NY, dtype=jnp.float32) / NY).reshape(1, -1, 1)
    along_z = (jnp.arange(NZ, dtype=jnp.float32) / NZ).reshape(1, 1, -1)
    base = jnp.clip(jax.random.normal(key, (REPS, NX, NY, NZ), jnp.float32), -6.0, 6.0)
    spread = 3.0 ** along_x * 1.7 ** along_y * 1.7 ** along_z
    return base * spread[None]


def place_ends(drawn, rng, smallest, top_value):
    longest = drawn.shape.index(max(drawn.shape))
    spots = []
    for shift in (0, 1):
        where = [jax.random.randint(jax.random.fold_in(rng, axis), (), 0, length) for axis, length in enumerate(drawn.shape)]
        where[longest] = (where[longest] + shift) % drawn.shape[longest]
        spots.append(tuple(where))
    return drawn.at[spots[0]].set(smallest).at[spots[1]].set(top_value)


def block_levels(stream_key, dims, split, low, largest):
    level = 1.0
    for dim, blocks in split:
        draws = jax.random.uniform(jax.random.fold_in(jax.random.fold_in(stream_key, 6), dim), (blocks,), jnp.float32, low / len(split), largest / len(split))
        level = level * jnp.repeat(jnp.exp(draws), dims[dim] // blocks).reshape((-1,) + (1,) * (len(dims) - 1 - dim))
    return level


def scatter_about(rng, extent, deviation, limit, shards=(), kind=jnp.bfloat16):
    entries = deviation * jax.random.normal(rng, extent, jnp.float32)
    if shards:
        entries = entries * block_levels(rng, extent, shards, -0.22, 0.18)
    return jnp.clip(entries, -limit, limit).astype(kind)


def setup_inputs(seed: int = 0) -> dict:
    keys = jax.random.split(jax.random.key(seed), 6)
    log_range = jnp.clip(0.7 + 1.3 * jax.random.uniform(keys[0], (NX, NY, NZ), jnp.float32) ** block_levels(keys[0], (NX, NY, NZ), ((0, 8), (1, 4), (2, 4)), -0.2, 0.2), 0.7, 2.0)
    state = draw_state(jax.random.fold_in(keys[5], 71), 0)
    adjoint_start = scatter_about(keys[2], (REPS, NX, NY, NZ), 0.05, 0.3, ((1, 8), (2, 4), (3, 4)), jnp.float32)
    obs_index = place_ends(jax.random.randint(keys[3], (REPS, N_GX, N_GY, N_GZ, NOBS), 0, CX * CY * CZ), jax.random.fold_in(keys[3], 1), 0, (CX * CY * CZ) - 1).astype(jnp.int32)
    obs_value = scatter_about(keys[4], (REPS, N_GX, N_GY, N_GZ, NOBS), 1.0, 6.0, ((1, 8), (2, 4), (3, 4)), jnp.float32)
    return {"log_range": log_range, "state": state, "adjoint_start": adjoint_start, "obs_index": obs_index, "obs_value": obs_value}


noise_var = 0.25


def stencil(field, kappa_sq):
    beside = jnp.roll(field, -1, 0) + jnp.roll(field, 1, 0)
    beside = beside + jnp.roll(field, -1, 1) + jnp.roll(field, 1, 1)
    beside = beside + jnp.roll(field, -1, 2) + jnp.roll(field, 1, 2)
    return (kappa_sq + 6.0) * field - beside


def reference(log_range, state, adjoint_start, obs_index, obs_value):
    kappa_sq = 4.0 * jnp.exp(-2.0 * log_range)
    block_x = (jnp.arange(N_GX, dtype=jnp.int32) * CX).reshape(-1, 1, 1, 1)
    block_y = (jnp.arange(N_GY, dtype=jnp.int32) * CY).reshape(1, -1, 1, 1)
    block_z = (jnp.arange(N_GZ, dtype=jnp.int32) * CZ).reshape(1, 1, -1, 1)
    total = NX * NY * NZ
    gradient = jnp.zeros((NX, NY, NZ), jnp.float32)
    adjoints = []
    for replica in range(REPS):
        local = obs_index[replica].astype(jnp.int32)
        first = local // (CY * CZ) + block_x
        second = (local // CZ) % CY + block_y
        third = local % CZ + block_z
        global_cell = ((first * NY + second) * NZ + third).reshape(-1).astype(jnp.int32)
        field = state[replica]
        misfit = field.reshape(-1)[global_cell] - obs_value[replica].reshape(-1)
        obs_weight = jnp.zeros((total,), jnp.float32).at[global_cell].add(1.0 / noise_var).reshape(NX, NY, NZ)
        right_side = jnp.zeros((total,), jnp.float32).at[global_cell].add(-misfit / noise_var).reshape(NX, NY, NZ)

        def system(vector):
            return stencil(stencil(vector, kappa_sq), kappa_sq) + obs_weight * vector

        adjoint = adjoint_start[replica]
        residual = right_side - system(adjoint)
        direction = residual
        norm_now = jnp.sum(residual * residual)
        for iteration in range(ITERS):
            image = system(direction)
            step_size = norm_now / jnp.sum(direction * image)
            adjoint = adjoint + step_size * direction
            if iteration + 1 < ITERS:
                residual = residual - step_size * image
                norm_next = jnp.sum(residual * residual)
                direction = residual + (norm_next / norm_now) * direction
                norm_now = norm_next
        state_image = stencil(field, kappa_sq)
        adjoint_image = stencil(adjoint, kappa_sq)
        gradient = gradient + (-2.0 * kappa_sq * (adjoint * state_image + adjoint_image * field))
        adjoints.append(adjoint)
    return gradient, jnp.stack(adjoints, 0)
```

```python
import functools

import jax
import jax.numpy as jnp
from jax import lax
from jax.experimental import pallas as pl
from jax.experimental.pallas import tpu as pltpu
from jax.sharding import PartitionSpec as P

ITERS = 4
SETS = 2
LANES = 128
TOP = 8
MESH = pl.DeviceIdType.MESH
INV_NOISE = 4.0


def kernel(
    sizes,
    lr_hbm, st_hbm, x0_hbm, index_ref, value_ref,
    grad_ref, adj_ref,
    kap, fp, ft, fs, xx, ax, pp, ap, ss, qq, ww, bb, ast,
    ysp, yst, yss, zsp, zst, zss, yrp, yrt, yrs, zrp, zrt, zrs,
    onehot_lo, onehot_hi, ar1, ar2, mine1, mine2,
    send_sem, recv_sem, ar_send, ar_recv1, ar_recv2, local_sem,
):
    gx_n, gy_n, gz_n = sizes
    nx, ny = kap.shape[0], kap.shape[1]
    yb_n = ny // 8
    gx, gy, gz = lax.axis_index("gx"), lax.axis_index("gy"), lax.axis_index("gz")

    def around(dx, dy, dz):
        return (
            lax.rem(gx + dx + gx_n, gx_n),
            lax.rem(gy + dy + gy_n, gy_n),
            lax.rem(gz + dz + gz_n, gz_n),
        )

    plane = [(0, dy, dz) for dy in range(gy_n) for dz in range(gz_n) if (dy, dz) != (0, 0)]
    column = [(dx, 0, 0) for dx in range(1, gx_n)]

    inner = (slice(None), pl.ds(1, nx), pl.ds(TOP, ny), slice(None))
    loads = [
        pltpu.make_async_copy(x0_hbm, fp.at[inner], local_sem.at[0]),
        pltpu.make_async_copy(st_hbm, fs.at[inner], local_sem.at[1]),
        pltpu.make_async_copy(lr_hbm, kap, local_sem.at[2]),
        pltpu.make_async_copy(x0_hbm, xx, local_sem.at[3]),
    ]
    for load in loads:
        load.start()

    barrier = pltpu.get_barrier_semaphore()
    for offset in plane + column:
        pl.semaphore_signal(barrier, inc=1, device_id=around(*offset), device_id_type=MESH)

    lane = lax.broadcasted_iota(jnp.int32, (8, LANES), 1)
    sub = lax.broadcasted_iota(jnp.int32, (8, LANES), 0)
    pair = lane // 2
    even = lane % 2 == 0
    zero = jnp.zeros((8, LANES), jnp.float32)

    def faces(kind, field, ys, zs, yr, zr):
        moves = [
            (field.at[:, nx, pl.ds(TOP, ny), :], field.at[:, 0, pl.ds(TOP, ny), :], (1, 0, 0)),
            (field.at[:, 1, pl.ds(TOP, ny), :], field.at[:, nx + 1, pl.ds(TOP, ny), :], (-1, 0, 0)),
            (ys.at[1], yr.at[0], (0, 1, 0)),
            (ys.at[0], yr.at[1], (0, -1, 0)),
            (zs, zr.at[0], (0, 0, 1)),
            (zs, zr.at[1], (0, 0, -1)),
        ]
        return [
            pltpu.make_async_remote_copy(
                src_ref=src, dst_ref=dst, send_sem=send_sem.at[kind, k], recv_sem=recv_sem.at[kind, k],
                device_id=around(*offset), device_id_type=MESH,
            )
            for k, (src, dst, offset) in enumerate(moves)
        ]

    def start(copies):
        for k in (4, 5, 2, 3, 0, 1):
            copies[k].start()

    def keep_rows(ys, s, x, yb, tile):
        if yb == 0:
            ys[0, s, pl.ds(x, 1), :] = tile[0:1, :]
        if yb == yb_n - 1:
            ys[1, s, pl.ds(x, 1), :] = tile[7:8, :]

    def packed(acc, s, x, tile):
        j = s * nx + x
        return jnp.where(pair == j, pltpu.roll(tile, 2 * j + 1, 1), acc)

    def put_packed(zs, acc):
        for yb in range(yb_n):
            zs[8 * yb : 8 * yb + 8, :] = acc[yb]

    def sweep(body, carry, lo, hi, unroll=1):
        return lax.fori_loop(lo, hi, body, carry, unroll=unroll)

    def face_pass(field, ys, zs):
        def body(x, acc):
            acc = list(acc)
            for s in range(SETS):
                for yb in range(yb_n):
                    tile = field[s, x + 1, TOP + 8 * yb : TOP + 8 * yb + 8, :]
                    keep_rows(ys, s, x, yb, tile)
                    acc[yb] = packed(acc[yb], s, x, tile)
            return tuple(acc)
        put_packed(zs, sweep(body, (zero,) * yb_n, 0, nx))

    def apply(field, copies, yr, zr, emit, carry, between=None):
        for k in (2, 3, 4, 5):
            copies[k].wait_recv()
        zc = [
            jnp.where(even, zr[0, 8 * yb : 8 * yb + 8, :], zr[1, 8 * yb : 8 * yb + 8, :])
            for yb in range(yb_n)
        ]

        def body(x, carry):
            for s in range(SETS):
                j = s * nx + x
                for yb in range(yb_n):
                    r = TOP + 8 * yb
                    c = field[s, x + 1, r : r + 8, :]
                    xs = field[s, x, r : r + 8, :] + field[s, x + 2, r : r + 8, :]
                    ym = field[s, x + 1, r - 1 : r + 7, :]
                    yp = field[s, x + 1, r + 1 : r + 9, :]
                    if yb == 0:
                        ym = jnp.where(sub == 0, yr[0, s, pl.ds(x, 1), :], ym)
                    if yb == yb_n - 1:
                        yp = jnp.where(sub == 7, yr[1, s, pl.ds(x, 1), :], yp)
                    h = pltpu.roll(zc[yb], LANES - 1 - 2 * j, 1)
                    zm = pltpu.roll(jnp.where(lane == LANES - 1, h, c), 1, 1)
                    zp = pltpu.roll(jnp.where(lane == 0, h, c), LANES - 1, 1)
                    beside = xs + (ym + yp) + (zm + zp)
                    out = (kap[x, 8 * yb : 8 * yb + 8, :] + 6.0) * c - beside
                    carry = emit(s, x, yb, c, out, carry)
            return carry

        carry = sweep(body, carry, 1, nx - 1)
        if between is not None:
            between()
        for k in (0, 1):
            copies[k].wait_recv()
        carry = body(0, carry)
        carry = body(nx - 1, carry)
        for copy in copies:
            copy.wait_send()
        return carry

    p_kind = (fp, ysp, zsp, yrp, zrp)
    t_kind = (ft, yst, zst, yrt, zrt)
    s_kind = (fs, yss, zss, yrs, zrs)

    loads[0].wait()
    face_pass(fp, ysp, zsp)
    pl.semaphore_wait(barrier, len(plane) + len(column))
    p_copies = faces(0, *p_kind)
    start(p_copies)
    loads[1].wait()
    face_pass(fs, yss, zss)
    s_copies = faces(2, *s_kind)
    start(s_copies)
    loads[2].wait()
    loads[3].wait()

    def kappa(x, _):
        kap[x] = 4.0 * jnp.exp(-2.0 * kap[x])
        return _
    sweep(kappa, 0, 0, nx)

    nobs = index_ref.shape[1]
    rows = onehot_hi.shape[0]
    step = 512
    planes = rows // ny

    def observe(s):
        for k in range(0, nobs, step):
            low = index_ref[s : s + 1, k : k + step] % LANES
            v = value_ref[s : s + 1, k : k + step]
            v1 = v.astype(jnp.bfloat16).astype(jnp.float32)
            v2 = (v - v1).astype(jnp.bfloat16).astype(jnp.float32)
            v3 = v - v1 - v2
            hit = lax.broadcasted_iota(jnp.int32, (LANES, step), 0) == low
            for n, weight in enumerate((jnp.ones_like(v), v1, v2, v3)):
                onehot_lo[LANES * n : LANES * (n + 1), k : k + step] = jnp.where(
                    hit, weight, 0.0
                ).astype(jnp.bfloat16)

        def body(m, _):
            for k in range(0, nobs, step):
                high = index_ref[s : s + 1, k : k + step] // LANES - m * rows
                onehot_hi[:, k : k + step] = jnp.where(
                    lax.broadcasted_iota(jnp.int32, (rows, step), 0) == high, 1.0, 0.0
                ).astype(jnp.bfloat16)
            sums = lax.dot_general(
                onehot_hi[...], onehot_lo[...], (((1,), (1,)), ((), ())),
                preferred_element_type=jnp.float32,
            )
            count = sums[:, :LANES].reshape(planes, ny, LANES)
            total = (sums[:, LANES : 2 * LANES] + sums[:, 2 * LANES : 3 * LANES]) + sums[:, 3 * LANES :]
            total = total.reshape(planes, ny, LANES)
            x = m * planes
            ww[s, pl.ds(x, planes)] = INV_NOISE * count
            bb[s, pl.ds(x, planes)] = INV_NOISE * (
                total - count * fs[s, pl.ds(x + 1, planes), TOP : TOP + ny, :]
            )
            return _
        sweep(body, 0, 0, nx // planes)

    observe(0)

    def rows_of(yb):
        return slice(8 * yb, 8 * yb + 8)

    def inner_rows(yb):
        return slice(TOP + 8 * yb, TOP + 8 * yb + 8)

    def emit_start(s, x, yb, c, out, acc):
        ft[s, x + 1, inner_rows(yb), :] = out
        ax[s, x, rows_of(yb), :] = out
        keep_rows(yst, s, x, yb, out)
        acc = list(acc)
        acc[yb] = packed(acc[yb], s, x, out)
        return tuple(acc)

    acc = apply(fp, p_copies, yrp, zrp, emit_start, (zero,) * yb_n)
    put_packed(zst, acc)
    t_copies = faces(1, *t_kind)
    start(t_copies)

    observe(1)

    def emit_state(s, x, yb, c, out, carry):
        ast[s, x, rows_of(yb), :] = out
        return carry
    apply(fs, s_copies, yrs, zrs, emit_state, 0)

    def emit_residual(s, x, yb, c, out, acc):
        v = fp[s, x + 1, inner_rows(yb), :]
        r = bb[s, x, rows_of(yb), :] - (out + ww[s, x, rows_of(yb), :] * v)
        fp[s, x + 1, inner_rows(yb), :] = r
        keep_rows(ysp, s, x, yb, r)
        acc = list(acc)
        acc[yb] = packed(acc[yb], s, x, r)
        return tuple(acc)

    acc = apply(ft, t_copies, yrt, zrt, emit_residual, (zero,) * yb_n)
    put_packed(zsp, acc)
    p_copies = faces(0, *p_kind)
    start(p_copies)

    def emit_first(s, x, yb, c, out, carry):
        ft[s, x + 1, inner_rows(yb), :] = out
        keep_rows(yst, s, x, yb, out)
        acc, sums = list(carry[0]), list(carry[1])
        acc[yb] = packed(acc[yb], s, x, out)
        square = c * c
        sums[s] = sums[s] + square
        sums[SETS + s] = sums[SETS + s] + (out * out + ww[s, x, rows_of(yb), :] * square)
        return (tuple(acc), tuple(sums))

    def emit_second(s, x, yb, c, out, carry):
        qq[s, x, rows_of(yb), :] = out + ww[s, x, rows_of(yb), :] * fp[s, x + 1, inner_rows(yb), :]
        return carry

    me1 = gy * gz_n + gz
    me2 = gx
    lane_row = lax.broadcasted_iota(jnp.int32, (1, LANES), 1)

    def first_stage(i, sums):
        row = jnp.zeros((1, LANES), jnp.float32)
        for n, part in enumerate(sums):
            total = jnp.sum(jnp.sum(part, axis=0, keepdims=True), axis=1, keepdims=True)
            row = jnp.where(lane_row == n, total, row)
        mine1[i] = row
        ar1[i, me1] = row
        copies = [
            pltpu.make_async_remote_copy(
                src_ref=mine1.at[i], dst_ref=ar1.at[i, me1], send_sem=ar_send.at[k],
                recv_sem=ar_recv1.at[i, k], device_id=around(*offset), device_id_type=MESH,
            )
            for k, offset in enumerate(plane)
        ]
        for copy in copies:
            copy.start()
        return copies

    def second_stage(i, copies):
        for copy in copies:
            copy.wait_recv()
        row = jnp.sum(ar1[i], axis=0)
        mine2[i] = row
        ar2[i, me2] = row
        later = [
            pltpu.make_async_remote_copy(
                src_ref=mine2.at[i], dst_ref=ar2.at[i, me2], send_sem=ar_send.at[len(plane) + k],
                recv_sem=ar_recv2.at[i, k], device_id=around(*offset), device_id_type=MESH,
            )
            for k, offset in enumerate(column)
        ]
        for copy in later:
            copy.start()
        return later

    def last_stage(i, copies, later):
        for copy in later:
            copy.wait_recv()
        row = jnp.sum(ar2[i], axis=0)
        for copy in copies + later:
            copy.wait_send()
        return [
            jnp.sum(jnp.where(lane_row == n, row, 0.0), axis=1, keepdims=True) for n in range(2 * SETS)
        ]

    norm_was = step_was = None
    for i in range(ITERS):
        acc, sums = apply(
            fp, p_copies, yrp, zrp, emit_first, ((zero,) * yb_n, (zero,) * (2 * SETS))
        )
        put_packed(zst, acc)
        copies = first_stage(i, sums)
        if i + 1 < ITERS:
            t_copies = faces(1, *t_kind)
            start(t_copies)
            box = []
            apply(ft, t_copies, yrt, zrt, emit_second, 0, lambda: box.append(second_stage(i, copies)))
            later = box[0]
        else:
            later = second_stage(i, copies)
        totals = last_stage(i, copies, later)
        norm, product = totals[:SETS], totals[SETS:]
        if i == 0:
            ratio = [None] * SETS
            size = [n / d for n, d in zip(norm, product)]
        else:
            ratio = [n / w for n, w in zip(norm, norm_was)]
            size = [n / (d - b * n / a) for n, d, b, a in zip(norm, product, ratio, step_was)]
        norm_was, step_was = norm, size
        beta = [None if b is None else jnp.broadcast_to(b, (8, LANES)) for b in ratio]
        alpha = [jnp.broadcast_to(a, (8, LANES)) for a in size]

        if i + 1 < ITERS:
            def advance(x, acc):
                acc = list(acc)
                for s in range(SETS):
                    for yb in range(yb_n):
                        rows_ = rows_of(yb)
                        r = fp[s, x + 1, inner_rows(yb), :]
                        p, image = r, qq[s, x, rows_, :]
                        if i > 0:
                            p = r + beta[s] * pp[s, x, rows_, :]
                            image = image + beta[s] * ss[s, x, rows_, :]
                        pp[s, x, rows_, :] = p
                        ss[s, x, rows_, :] = image
                        r = r - alpha[s] * image
                        fp[s, x + 1, inner_rows(yb), :] = r
                        keep_rows(ysp, s, x, yb, r)
                        acc[yb] = packed(acc[yb], s, x, r)
                return tuple(acc)
            put_packed(zsp, sweep(advance, (zero,) * yb_n, 0, nx))
            p_copies = faces(0, *p_kind)
            start(p_copies)

            def settle(x, _):
                for s in range(SETS):
                    for yb in range(yb_n):
                        rows_ = rows_of(yb)
                        applied = ft[s, x + 1, inner_rows(yb), :]
                        if i > 0:
                            applied = applied + beta[s] * ap[s, x, rows_, :]
                        ap[s, x, rows_, :] = applied
                        ax[s, x, rows_, :] += alpha[s] * applied
                        xx[s, x, rows_, :] += alpha[s] * pp[s, x, rows_, :]
                return _
            sweep(settle, 0, 0, nx)
        else:
            def finish(x, _):
                for yb in range(yb_n):
                    rows_ = rows_of(yb)
                    total = zero
                    for s in range(SETS):
                        p = fp[s, x + 1, inner_rows(yb), :] + beta[s] * pp[s, x, rows_, :]
                        applied = ft[s, x + 1, inner_rows(yb), :] + beta[s] * ap[s, x, rows_, :]
                        adjoint = xx[s, x, rows_, :] + alpha[s] * p
                        applied = ax[s, x, rows_, :] + alpha[s] * applied
                        adj_ref[s, x, rows_, :] = adjoint
                        total = total + (
                            adjoint * ast[s, x, rows_, :] + applied * fs[s, x + 1, inner_rows(yb), :]
                        )
                    grad_ref[x, rows_, :] = -2.0 * kap[x, rows_, :] * total
                return _
            sweep(finish, 0, 0, nx)


def on_device(sizes, log_range, state, adjoint_start, obs_index, obs_value):
    nx, ny, nz = log_range.shape
    nobs = obs_index.shape[-1]
    f32 = jnp.float32
    field = pltpu.VMEM((SETS, nx, ny, nz), f32)
    padded = pltpu.VMEM((SETS, nx + 2, ny + 2 * TOP, nz), f32)
    yface = pltpu.VMEM((2, SETS, nx, nz), f32)
    zsent = pltpu.VMEM((ny, LANES), f32)
    zgot = pltpu.VMEM((2, ny, LANES), f32)
    group = sizes[1] * sizes[2]
    vmem = pl.BlockSpec(memory_space=pltpu.VMEM)
    hbm = pl.BlockSpec(memory_space=pl.ANY)
    dma = pltpu.SemaphoreType.DMA
    return pl.pallas_call(
        functools.partial(kernel, sizes),
        out_shape=(
            jax.ShapeDtypeStruct((nx, ny, nz), f32),
            jax.ShapeDtypeStruct((SETS, nx, ny, nz), f32),
        ),
        in_specs=[hbm, hbm, hbm, vmem, vmem],
        out_specs=(vmem, vmem),
        scratch_shapes=[
            pltpu.VMEM((nx, ny, nz), f32),
            padded, padded, padded,
            field, field, field, field, field, field, field, field, field,
            yface, yface, yface, zsent, zsent, zsent, yface, yface, yface, zgot, zgot, zgot,
            pltpu.VMEM((4 * LANES, nobs), jnp.bfloat16),
            pltpu.VMEM((256, nobs), jnp.bfloat16),
            pltpu.VMEM((ITERS, group, 1, LANES), f32),
            pltpu.VMEM((ITERS, sizes[0], 1, LANES), f32),
            pltpu.VMEM((ITERS, 1, LANES), f32),
            pltpu.VMEM((ITERS, 1, LANES), f32),
            dma((3, 6)), dma((3, 6)),
            dma((group + sizes[0] - 2,)),
            dma((ITERS, group - 1)), dma((ITERS, sizes[0] - 1)),
            dma((4,)),
        ],
        compiler_params=pltpu.CompilerParams(
            collective_id=0, has_side_effects=True, vmem_limit_bytes=60 * 1024 * 1024
        ),
    )(
        log_range, state, adjoint_start,
        obs_index.reshape(SETS, nobs), obs_value.reshape(SETS, nobs),
    )


def solution(mesh):
    sizes = (mesh.shape["gx"], mesh.shape["gy"], mesh.shape["gz"])
    whole, per_set = P("gx", "gy", "gz"), P(None, "gx", "gy", "gz")
    obs = P(None, "gx", "gy", "gz", None)
    return jax.shard_map(
        functools.partial(on_device, sizes), mesh=mesh,
        in_specs=(whole, per_set, per_set, obs, obs), out_specs=(whole, per_set), check_vma=False,
    )
```

```python
import functools

import jax
import jax.numpy as jnp
from jax import lax
from jax.experimental import pallas as pl
from jax.experimental.pallas import tpu as pltpu
from jax.sharding import PartitionSpec as P

ITERS = 4
SETS = 2
LANES = 128
TOP = 8
MESH = pl.DeviceIdType.MESH
INTERIOR = 6
WHOLE = 8
INV_NOISE = 4.0


def kernel(
    sizes,
    lr_hbm, st_hbm, x0_hbm, index_ref, value_ref,
    grad_ref, adj_ref,
    kap, fp, ft, fs, part, xx, ax, pp, ap, ss, sa, rr, ra, zz, ww, bb, ast,
    ysp, yst, yss, zsp, zst, zss, yrp, yrt, yrs, zrp, zrt, zrs,
    onehot_lo, onehot_hi, ar1, ar2, mine1, mine2,
    send_sem, recv_sem, ar_send, ar_recv1, ar_recv2, local_sem,
):
    gx_n, gy_n, gz_n = sizes
    nx, ny = kap.shape[0], kap.shape[1]
    yb_n = ny // 8
    gx, gy, gz = lax.axis_index("gx"), lax.axis_index("gy"), lax.axis_index("gz")

    def around(dx, dy, dz):
        return (
            lax.rem(gx + dx + gx_n, gx_n),
            lax.rem(gy + dy + gy_n, gy_n),
            lax.rem(gz + dz + gz_n, gz_n),
        )

    plane = [(0, dy, dz) for dy in range(gy_n) for dz in range(gz_n) if (dy, dz) != (0, 0)]
    column = [(dx, 0, 0) for dx in range(1, gx_n)]

    inner = (slice(None), pl.ds(1, nx), pl.ds(TOP, ny), slice(None))
    loads = [
        pltpu.make_async_copy(x0_hbm, fp.at[inner], local_sem.at[0]),
        pltpu.make_async_copy(st_hbm, fs.at[inner], local_sem.at[1]),
        pltpu.make_async_copy(lr_hbm, kap, local_sem.at[2]),
        pltpu.make_async_copy(x0_hbm, xx, local_sem.at[3]),
    ]
    for load in loads:
        load.start()

    barrier = pltpu.get_barrier_semaphore()
    for offset in plane + column:
        pl.semaphore_signal(barrier, inc=1, device_id=around(*offset), device_id_type=MESH)

    lane = lax.broadcasted_iota(jnp.int32, (8, LANES), 1)
    sub = lax.broadcasted_iota(jnp.int32, (8, LANES), 0)
    pair = lane // 2
    even = lane % 2 == 0
    zero = jnp.zeros((8, LANES), jnp.float32)

    def faces(kind, field, ys, zs, yr, zr):
        moves = [
            (field.at[:, nx, pl.ds(TOP, ny), :], field.at[:, 0, pl.ds(TOP, ny), :], (1, 0, 0)),
            (field.at[:, 1, pl.ds(TOP, ny), :], field.at[:, nx + 1, pl.ds(TOP, ny), :], (-1, 0, 0)),
            (ys.at[1], yr.at[0], (0, 1, 0)),
            (ys.at[0], yr.at[1], (0, -1, 0)),
            (zs, zr.at[0], (0, 0, 1)),
            (zs, zr.at[1], (0, 0, -1)),
        ]
        return [
            pltpu.make_async_remote_copy(
                src_ref=src, dst_ref=dst, send_sem=send_sem.at[kind, k], recv_sem=recv_sem.at[kind, k],
                device_id=around(*offset), device_id_type=MESH,
            )
            for k, (src, dst, offset) in enumerate(moves)
        ]

    def start(copies):
        for k in (4, 5, 2, 3, 0, 1):
            copies[k].start()

    def keep_rows(ys, s, x, yb, tile):
        if yb == 0:
            ys[0, s, pl.ds(x, 1), :] = tile[0:1, :]
        if yb == yb_n - 1:
            ys[1, s, pl.ds(x, 1), :] = tile[7:8, :]

    def packed(acc, s, x, tile):
        j = s * nx + x
        return jnp.where(pair == j, pltpu.roll(tile, 2 * j + 1, 1), acc)

    def put_packed(zs, acc):
        for yb in range(yb_n):
            zs[8 * yb : 8 * yb + 8, :] = acc[yb]

    def sweep(body, carry, lo, hi, unroll=1):
        def several(n, carry):
            for k in range(unroll):
                carry = body(lo + n * unroll + k, carry)
            return carry
        return lax.fori_loop(0, (hi - lo) // unroll, several, carry)

    def face_pass(field, ys, zs):
        def body(x, acc):
            acc = list(acc)
            for s in range(SETS):
                for yb in range(yb_n):
                    tile = field[s, x + 1, TOP + 8 * yb : TOP + 8 * yb + 8, :]
                    keep_rows(ys, s, x, yb, tile)
                    acc[yb] = packed(acc[yb], s, x, tile)
            return tuple(acc)
        put_packed(zs, sweep(body, (zero,) * yb_n, 0, nx, WHOLE))

    def rows_of(yb):
        return slice(8 * yb, 8 * yb + 8)

    def inner_rows(yb):
        return slice(TOP + 8 * yb, TOP + 8 * yb + 8)

    sides = (lane == 0) | (lane == LANES - 1)

    def apply(field, copies, yr, zr, emit, carry, gap=None, mid=None, part=part):
        def partial(x, _, lower=True, upper=True):
            for s in range(SETS):
                for yb in range(yb_n):
                    r = TOP + 8 * yb
                    c = field[s, x + 1, r : r + 8, :]
                    ym = field[s, x + 1, r - 1 : r + 7, :]
                    yp = field[s, x + 1, r + 1 : r + 9, :]
                    if yb == 0:
                        ym = jnp.where(sub == 0, 0.0, ym)
                    if yb == yb_n - 1:
                        yp = jnp.where(sub == 7, 0.0, yp)
                    zm = jnp.where(lane == 0, 0.0, pltpu.roll(c, 1, 1))
                    zp = jnp.where(lane == LANES - 1, 0.0, pltpu.roll(c, LANES - 1, 1))
                    beside = (ym + yp) + (zm + zp)
                    if lower:
                        beside = beside + field[s, x, r : r + 8, :]
                    if upper:
                        beside = beside + field[s, x + 2, r : r + 8, :]
                    part[s, x, rows_of(yb), :] = (kap[x, rows_of(yb), :] + 6.0) * c - beside
            return _

        partial(0, 0, lower=False)
        partial(nx - 1, 0, upper=False)
        sweep(partial, 0, 1, nx - 1, INTERIOR)
        if gap is not None:
            gap()
        for k in (2, 3, 4, 5):
            copies[k].wait_recv()
        zc = [
            jnp.where(even, zr[0, rows_of(yb), :], pltpu.roll(zr[1, rows_of(yb), :], LANES - 2, 1))
            for yb in range(yb_n)
        ]

        def complete(x, carry, slab=None):
            for s in range(SETS):
                shift = lax.rem(LANES - 2 * (s * nx + x), LANES)
                for yb in range(yb_n):
                    out = part[s, x, rows_of(yb), :]
                    out = out - jnp.where(sides, pltpu.roll(zc[yb], shift, 1), 0.0)
                    if yb == 0:
                        out = out - jnp.where(sub == 0, yr[0, s, pl.ds(x, 1), :], 0.0)
                    if yb == yb_n - 1:
                        out = out - jnp.where(sub == 7, yr[1, s, pl.ds(x, 1), :], 0.0)
                    if slab is not None:
                        out = out - field[s, slab, inner_rows(yb), :]
                    carry = emit(s, x, yb, out, carry)
            return carry

        carry = sweep(complete, carry, 1, nx - 1, INTERIOR)
        if mid is not None:
            mid()
        for k in (0, 1):
            copies[k].wait_recv()
        carry = complete(0, carry, 0)
        carry = complete(nx - 1, carry, nx + 1)
        for copy in copies:
            copy.wait_send()
        return carry

    p_kind = (fp, ysp, zsp, yrp, zrp)
    t_kind = (ft, yst, zst, yrt, zrt)
    s_kind = (fs, yss, zss, yrs, zrs)

    def kappa(x, _):
        kap[x] = 4.0 * jnp.exp(-2.0 * kap[x])
        return _

    nobs = index_ref.shape[2]
    rows = onehot_hi.shape[0]
    step = 512
    planes = rows // ny

    def build(s):
        for k in range(0, nobs, step):
            low = index_ref[s, :, k : k + step] % LANES
            v = value_ref[s, :, k : k + step]
            v1 = v.astype(jnp.bfloat16).astype(jnp.float32)
            v2 = (v - v1).astype(jnp.bfloat16).astype(jnp.float32)
            v3 = v - v1 - v2
            hit = lax.broadcasted_iota(jnp.int32, (LANES, step), 0) == low
            for n, weight in enumerate((jnp.ones_like(v), v1, v2, v3)):
                onehot_lo[LANES * n : LANES * (n + 1), k : k + step] = jnp.where(
                    hit, weight, 0.0
                ).astype(jnp.bfloat16)

    def observe(s, lo, hi):
        def body(m, _):
            for k in range(0, nobs, step):
                high = index_ref[s, :, k : k + step] // LANES - m * rows
                onehot_hi[:, k : k + step] = jnp.where(
                    lax.broadcasted_iota(jnp.int32, (rows, step), 0) == high, 1.0, 0.0
                ).astype(jnp.bfloat16)
            sums = lax.dot_general(
                onehot_hi[...], onehot_lo[...], (((1,), (1,)), ((), ())),
                preferred_element_type=jnp.float32,
            )
            count = sums[:, :LANES].reshape(planes, ny, LANES)
            total = (sums[:, LANES : 2 * LANES] + sums[:, 2 * LANES : 3 * LANES]) + sums[:, 3 * LANES :]
            total = total.reshape(planes, ny, LANES)
            x = m * planes
            ww[s, pl.ds(x, planes)] = INV_NOISE * count
            bb[s, pl.ds(x, planes)] = INV_NOISE * (
                total - count * fs[s, pl.ds(x + 1, planes), TOP : TOP + ny, :]
            )
            return _
        sweep(body, 0, lo, hi)

    me1 = gy * gz_n + gz
    me2 = gx
    lane_row = lax.broadcasted_iota(jnp.int32, (1, LANES), 1)

    def first_stage(i, sums):
        row = jnp.zeros((1, LANES), jnp.float32)
        for n, share in enumerate(sums):
            total = jnp.sum(jnp.sum(share, axis=0, keepdims=True), axis=1, keepdims=True)
            row = jnp.where(lane_row == n, total, row)
        mine1[i] = row
        ar1[i, me1] = row
        copies = [
            pltpu.make_async_remote_copy(
                src_ref=mine1.at[i], dst_ref=ar1.at[i, me1], send_sem=ar_send.at[k],
                recv_sem=ar_recv1.at[i, k], device_id=around(*offset), device_id_type=MESH,
            )
            for k, offset in enumerate(plane)
        ]
        for copy in copies:
            copy.start()
        return copies

    def second_stage(i, copies):
        for copy in copies:
            copy.wait_recv()
        row = jnp.sum(ar1[i], axis=0)
        mine2[i] = row
        ar2[i, me2] = row
        later = [
            pltpu.make_async_remote_copy(
                src_ref=mine2.at[i], dst_ref=ar2.at[i, me2], send_sem=ar_send.at[len(plane) + k],
                recv_sem=ar_recv2.at[i, k], device_id=around(*offset), device_id_type=MESH,
            )
            for k, offset in enumerate(column)
        ]
        for copy in later:
            copy.start()
        return copies + later

    def last_stage(i, copies):
        for copy in copies[len(plane) :]:
            copy.wait_recv()
        row = jnp.sum(ar2[i], axis=0)
        for copy in copies:
            copy.wait_send()
        return [
            jnp.sum(jnp.where(lane_row == n, row, 0.0), axis=1, keepdims=True) for n in range(2 * SETS)
        ]

    sums_of = {}
    norm, size, alpha, beta = {}, {}, {}, {}

    def middle(i):
        sums_of[i] = second_stage(i, sums_of[i])

    def scalars(i):
        totals = last_stage(i, sums_of[i])
        norm[i], product = totals[:SETS], totals[SETS:]
        if i == 0:
            size[i] = [n / d for n, d in zip(norm[i], product)]
        else:
            ratio = [n / w for n, w in zip(norm[i], norm[i - 1])]
            size[i] = [n / (d - b * n / a) for n, d, b, a in zip(norm[i], product, ratio, size[i - 1])]
            beta[i] = [jnp.broadcast_to(b, (8, LANES)) for b in ratio]
        alpha[i] = [jnp.broadcast_to(a, (8, LANES)) for a in size[i]]

    def advance(i):
        scalars(i)

        def body(x, sums):
            sums = list(sums)
            for s in range(SETS):
                for yb in range(yb_n):
                    at = (s, x, rows_of(yb), slice(None))
                    r, r_image = rr[at], ra[at]
                    p, p_image = r, r_image
                    q = fp[s, x + 1, inner_rows(yb), :]
                    q_image = ft[s, x + 1, inner_rows(yb), :]
                    if i > 0:
                        p = p + beta[i][s] * pp[at]
                        p_image = p_image + beta[i][s] * ap[at]
                        q = q + beta[i][s] * ss[at]
                        q_image = q_image + beta[i][s] * sa[at]
                    pp[at], ap[at] = p, p_image
                    if i + 2 < ITERS:
                        ss[at], sa[at] = q, q_image
                    xx[at] += alpha[i][s] * p
                    ax[at] += alpha[i][s] * p_image
                    r = r - alpha[i][s] * q
                    r_image = r_image - alpha[i][s] * q_image
                    rr[at], ra[at] = r, r_image
                    square = r * r
                    sums[s] = sums[s] + square
                    sums[SETS + s] = sums[SETS + s] + (r_image * r_image + ww[at] * square)
            return tuple(sums)
        sums_of[i + 1] = first_stage(i + 1, sweep(body, (zero,) * (2 * SETS), 0, nx, 2))

    no_faces = (zero,) * yb_n

    def sent(ys, s, x, yb, tile, acc):
        keep_rows(ys, s, x, yb, tile)
        acc = list(acc)
        acc[yb] = packed(acc[yb], s, x, tile)
        return tuple(acc)

    def send(kind, parts, acc):
        put_packed(parts[2], acc)
        copies = faces(kind, *parts)
        start(copies)
        return copies

    loads[0].wait()
    face_pass(fp, ysp, zsp)
    loads[2].wait()
    sweep(kappa, 0, 0, nx)
    loads[1].wait()
    face_pass(fs, yss, zss)
    loads[3].wait()
    build(0)
    observe(0, 0, 2)
    pl.semaphore_wait(barrier, len(plane) + len(column))
    p_copies = faces(0, *p_kind)
    start(p_copies)
    s_copies = faces(2, *s_kind)
    start(s_copies)

    def gap():
        observe(0, 2, 4)
        build(1)

    def emit_start(s, x, yb, out, acc):
        ft[s, x + 1, inner_rows(yb), :] = out
        ax[s, x, rows_of(yb), :] = out
        return sent(yst, s, x, yb, out, acc)

    t_copies = send(1, t_kind, apply(fp, p_copies, yrp, zrp, emit_start, no_faces, gap))

    def gap():
        observe(1, 0, 4)

    def emit_residual(s, x, yb, out, acc):
        at = (s, x, rows_of(yb), slice(None))
        r = bb[at] - (out + ww[at] * xx[at])
        rr[at] = r
        fp[s, x + 1, inner_rows(yb), :] = r
        return sent(ysp, s, x, yb, r, acc)

    p_copies = send(0, p_kind, apply(ft, t_copies, yrt, zrt, emit_residual, no_faces, gap))

    def emit_state(s, x, yb, out, carry):
        ast[s, x, rows_of(yb), :] = out
        return carry

    def emit_first(s, x, yb, out, carry):
        at = (s, x, rows_of(yb), slice(None))
        ft[s, x + 1, inner_rows(yb), :] = out
        ra[at] = out
        acc, sums = carry[0], list(carry[1])
        square = rr[at] * rr[at]
        sums[s] = sums[s] + square
        sums[SETS + s] = sums[SETS + s] + (out * out + ww[at] * square)
        return (sent(yst, s, x, yb, out, acc), tuple(sums))

    acc, sums = apply(fp, p_copies, yrp, zrp, emit_first, (no_faces, (zero,) * (2 * SETS)))
    sums_of[0] = first_stage(0, sums)
    t_copies = send(1, t_kind, acc)

    def emit_image(s, x, yb, out, acc):
        at = (s, x, rows_of(yb), slice(None))
        w = out + ww[at] * rr[at]
        fp[s, x + 1, inner_rows(yb), :] = w
        return sent(ysp, s, x, yb, w, acc)

    acc = apply(
        ft, t_copies, yrt, zrt, emit_image, no_faces,
        lambda: apply(fs, s_copies, yrs, zrs, emit_state, 0, part=ast), lambda: middle(0),
    )
    p_copies = send(0, p_kind, acc)

    for i in range(ITERS - 1):
        last = i + 2 == ITERS

        def emit_inner(s, x, yb, out, acc):
            ft[s, x + 1, inner_rows(yb), :] = out
            return acc if last else sent(yst, s, x, yb, out, acc)

        def emit_outer(s, x, yb, out, acc):
            at = (s, x, rows_of(yb), slice(None))
            w = fp[s, x + 1, inner_rows(yb), :]
            z = out + ww[at] * w
            if i > 0:
                z = z + beta[i][s] * zz[at]
            if i + 3 < ITERS:
                zz[at] = z
            w = w - alpha[i][s] * z
            fp[s, x + 1, inner_rows(yb), :] = w
            return sent(ysp, s, x, yb, w, acc)

        acc = apply(
            fp, p_copies, yrp, zrp, emit_inner, no_faces, None,
            None if i == 0 else functools.partial(middle, i),
        )
        if last:
            advance(i)
        else:
            t_copies = send(1, t_kind, acc)
            acc = apply(
                ft, t_copies, yrt, zrt, emit_outer, no_faces, functools.partial(advance, i)
            )
            p_copies = send(0, p_kind, acc)

    i = ITERS - 1
    middle(i)
    scalars(i)

    def finish(x, _):
        for yb in range(yb_n):
            total = zero
            for s in range(SETS):
                at = (s, x, rows_of(yb), slice(None))
                p = rr[at] + beta[i][s] * pp[at]
                p_image = ra[at] + beta[i][s] * ap[at]
                adjoint = xx[at] + alpha[i][s] * p
                image = ax[at] + alpha[i][s] * p_image
                adj_ref[at] = adjoint
                total = total + (adjoint * ast[at] + image * fs[s, x + 1, inner_rows(yb), :])
            grad_ref[x, rows_of(yb), :] = -2.0 * kap[x, rows_of(yb), :] * total
        return _
    sweep(finish, 0, 0, nx, 2)


def on_device(sizes, log_range, state, adjoint_start, obs_index, obs_value):
    nx, ny, nz = log_range.shape
    nobs = obs_index.shape[-1]
    f32 = jnp.float32
    field = pltpu.VMEM((SETS, nx, ny, nz), f32)
    padded = pltpu.VMEM((SETS, nx + 2, ny + 2 * TOP, nz), f32)
    yface = pltpu.VMEM((2, SETS, nx, nz), f32)
    zsent = pltpu.VMEM((ny, LANES), f32)
    zgot = pltpu.VMEM((2, ny, LANES), f32)
    group = sizes[1] * sizes[2]
    vmem = pl.BlockSpec(memory_space=pltpu.VMEM)
    hbm = pl.BlockSpec(memory_space=pl.ANY)
    dma = pltpu.SemaphoreType.DMA
    return pl.pallas_call(
        functools.partial(kernel, sizes),
        out_shape=(
            jax.ShapeDtypeStruct((nx, ny, nz), f32),
            jax.ShapeDtypeStruct((SETS, nx, ny, nz), f32),
        ),
        in_specs=[hbm, hbm, hbm, vmem, vmem],
        out_specs=(vmem, vmem),
        scratch_shapes=[
            pltpu.VMEM((nx, ny, nz), f32),
            padded, padded, padded,
            field, field, field, field, field, field, field, field, field, field, field, field, field,
            yface, yface, yface, zsent, zsent, zsent, yface, yface, yface, zgot, zgot, zgot,
            pltpu.VMEM((4 * LANES, nobs), jnp.bfloat16),
            pltpu.VMEM((256, nobs), jnp.bfloat16),
            pltpu.VMEM((ITERS, group, 1, LANES), f32),
            pltpu.VMEM((ITERS, sizes[0], 1, LANES), f32),
            pltpu.VMEM((ITERS, 1, LANES), f32),
            pltpu.VMEM((ITERS, 1, LANES), f32),
            dma((3, 6)), dma((3, 6)),
            dma((group + sizes[0] - 2,)),
            dma((ITERS, group - 1)), dma((ITERS, sizes[0] - 1)),
            dma((4,)),
        ],
        compiler_params=pltpu.CompilerParams(
            collective_id=0, has_side_effects=True, vmem_limit_bytes=60 * 1024 * 1024
        ),
    )(
        log_range, state, adjoint_start,
        obs_index.reshape(SETS, 1, nobs), obs_value.reshape(SETS, 1, nobs),
    )


def solution(mesh):
    sizes = (mesh.shape["gx"], mesh.shape["gy"], mesh.shape["gz"])
    whole, per_set = P("gx", "gy", "gz"), P(None, "gx", "gy", "gz")
    obs = P(None, "gx", "gy", "gz", None)
    return jax.shard_map(
        functools.partial(on_device, sizes), mesh=mesh,
        in_specs=(whole, per_set, per_set, obs, obs), out_specs=(whole, per_set), check_vma=False,
    )
```

```python
import functools

import jax
import jax.numpy as jnp
from jax import lax
from jax.experimental import pallas as pl
from jax.experimental.pallas import tpu as pltpu
from jax.sharding import PartitionSpec as P

ITERS = 4
SETS = 2
LANES = 128
TOP = 8
MESH = pl.DeviceIdType.MESH
INTERIOR = 10
WHOLE = 8
INV_NOISE = 4.0


def kernel(
    sizes,
    lr_hbm, st_hbm, x0_hbm, index_hbm, value_hbm,
    grad_ref, adj_ref,
    kap, fp, ft, fs, part, xx, ax, pp, ap, ss, sa, rr, ra, zz, ww, bb, ast,
    ysp, yst, yss, zsp, zst, zss, yrp, yrt, yrs, zrp, zrt, zrs,
    onehot_lo, onehot_hi, index_ref, value_ref, rows_all, mine,
    send_sem, recv_sem, sum_send, sum_recv, local_sem,
):
    gx_n, gy_n, gz_n = sizes
    nx, ny = kap.shape[0], kap.shape[1]
    yb_n = ny // 8
    gx, gy, gz = lax.axis_index("gx"), lax.axis_index("gy"), lax.axis_index("gz")

    def around(dx, dy, dz):
        return (
            lax.rem(gx + dx + gx_n, gx_n),
            lax.rem(gy + dy + gy_n, gy_n),
            lax.rem(gz + dz + gz_n, gz_n),
        )

    def length(offset):
        return sum(min(d, n - d) for d, n in zip(offset, sizes))

    others = [
        (dx, dy, dz) for dx in range(gx_n) for dy in range(gy_n) for dz in range(gz_n)
    ][1:]
    others.sort(key=length, reverse=True)

    inner = (slice(None), pl.ds(1, nx), pl.ds(TOP, ny), slice(None))
    loads = [
        pltpu.make_async_copy(x0_hbm, fp.at[inner], local_sem.at[0]),
        pltpu.make_async_copy(st_hbm, fs.at[inner], local_sem.at[1]),
        pltpu.make_async_copy(lr_hbm, kap, local_sem.at[2]),
        pltpu.make_async_copy(x0_hbm, xx, local_sem.at[3]),
        pltpu.make_async_copy(index_hbm, index_ref, local_sem.at[4]),
        pltpu.make_async_copy(value_hbm, value_ref, local_sem.at[5]),
    ]
    for load in loads:
        load.start()

    barrier = pltpu.get_barrier_semaphore()
    for offset in others:
        pl.semaphore_signal(barrier, inc=1, device_id=around(*offset), device_id_type=MESH)

    lane = lax.broadcasted_iota(jnp.int32, (8, LANES), 1)
    sub = lax.broadcasted_iota(jnp.int32, (8, LANES), 0)
    pair = lane // 2
    even = lane % 2 == 0
    zero = jnp.zeros((8, LANES), jnp.float32)

    def faces(kind, field, ys, zs, yr, zr):
        moves = [
            (field.at[:, nx, pl.ds(TOP, ny), :], field.at[:, 0, pl.ds(TOP, ny), :], (1, 0, 0)),
            (field.at[:, 1, pl.ds(TOP, ny), :], field.at[:, nx + 1, pl.ds(TOP, ny), :], (-1, 0, 0)),
            (ys.at[1], yr.at[0], (0, 1, 0)),
            (ys.at[0], yr.at[1], (0, -1, 0)),
            (zs, zr.at[0], (0, 0, 1)),
            (zs, zr.at[1], (0, 0, -1)),
        ]
        return [
            pltpu.make_async_remote_copy(
                src_ref=src, dst_ref=dst, send_sem=send_sem.at[kind, k], recv_sem=recv_sem.at[kind, k],
                device_id=around(*offset), device_id_type=MESH,
            )
            for k, (src, dst, offset) in enumerate(moves)
        ]

    def start(copies):
        for k in (4, 5, 2, 3, 0, 1):
            copies[k].start()

    def keep_rows(ys, s, x, yb, tile):
        if yb == 0:
            ys[0, s, pl.ds(x, 1), :] = tile[0:1, :]
        if yb == yb_n - 1:
            ys[1, s, pl.ds(x, 1), :] = tile[7:8, :]

    def packed(acc, s, x, tile):
        j = s * nx + x
        return jnp.where(pair == j, pltpu.roll(tile, 2 * j + 1, 1), acc)

    def put_packed(zs, acc):
        for yb in range(yb_n):
            zs[8 * yb : 8 * yb + 8, :] = acc[yb]

    def sweep(body, carry, lo, hi, unroll=1):
        def several(n, carry):
            for k in range(unroll):
                carry = body(lo + n * unroll + k, carry)
            return carry
        return lax.fori_loop(0, (hi - lo) // unroll, several, carry)

    def face_pass(field, ys, zs):
        def body(x, acc):
            acc = list(acc)
            for s in range(SETS):
                for yb in range(yb_n):
                    tile = field[s, x + 1, TOP + 8 * yb : TOP + 8 * yb + 8, :]
                    keep_rows(ys, s, x, yb, tile)
                    acc[yb] = packed(acc[yb], s, x, tile)
            return tuple(acc)
        put_packed(zs, sweep(body, (zero,) * yb_n, 0, nx, WHOLE))

    def rows_of(yb):
        return slice(8 * yb, 8 * yb + 8)

    def inner_rows(yb):
        return slice(TOP + 8 * yb, TOP + 8 * yb + 8)

    sides = (lane == 0) | (lane == LANES - 1)

    def apply(field, copies, yr, zr, emit, carry, gap=None, mid=None, part=part):
        def partial(x, _, lower=True, upper=True):
            for s in range(SETS):
                for yb in range(yb_n):
                    r = TOP + 8 * yb
                    c = field[s, x + 1, r : r + 8, :]
                    ym = field[s, x + 1, r - 1 : r + 7, :]
                    yp = field[s, x + 1, r + 1 : r + 9, :]
                    if yb == 0:
                        ym = jnp.where(sub == 0, 0.0, ym)
                    if yb == yb_n - 1:
                        yp = jnp.where(sub == 7, 0.0, yp)
                    zm = jnp.where(lane == 0, 0.0, pltpu.roll(c, 1, 1))
                    zp = jnp.where(lane == LANES - 1, 0.0, pltpu.roll(c, LANES - 1, 1))
                    beside = (ym + yp) + (zm + zp)
                    if lower:
                        beside = beside + field[s, x, r : r + 8, :]
                    if upper:
                        beside = beside + field[s, x + 2, r : r + 8, :]
                    part[s, x, rows_of(yb), :] = (kap[x, rows_of(yb), :] + 6.0) * c - beside
            return _

        partial(0, 0, lower=False)
        partial(nx - 1, 0, upper=False)
        sweep(partial, 0, 1, nx - 1, INTERIOR)
        if gap is not None:
            gap()
        for k in (2, 3, 4, 5):
            copies[k].wait_recv()
        zc = [
            jnp.where(even, zr[0, rows_of(yb), :], pltpu.roll(zr[1, rows_of(yb), :], LANES - 2, 1))
            for yb in range(yb_n)
        ]

        def complete(x, carry, slab=None):
            for s in range(SETS):
                shift = lax.rem(LANES - 2 * (s * nx + x), LANES)
                for yb in range(yb_n):
                    out = part[s, x, rows_of(yb), :]
                    out = out - jnp.where(sides, pltpu.roll(zc[yb], shift, 1), 0.0)
                    if yb == 0:
                        out = out - jnp.where(sub == 0, yr[0, s, pl.ds(x, 1), :], 0.0)
                    if yb == yb_n - 1:
                        out = out - jnp.where(sub == 7, yr[1, s, pl.ds(x, 1), :], 0.0)
                    if slab is not None:
                        out = out - field[s, slab, inner_rows(yb), :]
                    carry = emit(s, x, yb, out, carry)
            return carry

        carry = sweep(complete, carry, 1, nx - 1, INTERIOR)
        if mid is not None:
            mid()
        for k in (0, 1):
            copies[k].wait_recv()
        carry = complete(0, carry, 0)
        carry = complete(nx - 1, carry, nx + 1)
        for copy in copies:
            copy.wait_send()
        return carry

    p_kind = (fp, ysp, zsp, yrp, zrp)
    t_kind = (ft, yst, zst, yrt, zrt)
    s_kind = (fs, yss, zss, yrs, zrs)

    def kappa(x, _):
        kap[x] = 4.0 * jnp.exp(-2.0 * kap[x])
        return _

    nobs = index_ref.shape[2]
    rows = onehot_hi.shape[0]
    step = 512
    bf16 = jnp.bfloat16
    planes = rows // ny

    halves = 2
    rows_half = nx * ny // halves

    def spread(count, numbers, weights):
        hit = lax.broadcasted_iota(jnp.int32, (count, step), 0).astype(bf16) == numbers.astype(
            jnp.float32
        ).astype(bf16)
        return [jnp.where(hit, weight, jnp.zeros_like(weight)) for weight in weights]

    def build(s):
        for k in range(0, nobs, step):
            cell = index_ref[s, :, k : k + step]
            low = cell % LANES + cell // (rows_half * LANES) * LANES
            v = value_ref[s, :, k : k + step]
            v1 = v.astype(bf16)
            v2 = (v - v1.astype(jnp.float32)).astype(bf16)
            for n, tile in enumerate(spread(halves * LANES, low, (jnp.ones_like(v1), v1, v2))):
                onehot_lo[halves * LANES * n : halves * LANES * (n + 1), k : k + step] = tile

    def observe(s, lo, hi):
        def body(m, _):
            for k in range(0, nobs, step):
                high = index_ref[s, :, k : k + step] // LANES % rows_half
                for r in range(0, rows, 256):
                    ones = jnp.ones((1, step), bf16)
                    onehot_hi[r : r + 256, k : k + step] = spread(256, high - (m * rows + r), (ones,))[0]
            sums = lax.dot_general(
                onehot_hi[...], onehot_lo[...], (((1,), (1,)), ((), ())),
                preferred_element_type=jnp.float32,
            )
            for h in range(halves):
                count, high, low = (
                    sums[:, (halves * n + h) * LANES : (halves * n + h + 1) * LANES] for n in range(3)
                )
                count = count.reshape(planes, ny, LANES)
                total = (high + low).reshape(planes, ny, LANES)
                x = h * (nx // halves) + m * planes
                ww[s, pl.ds(x, planes)] = INV_NOISE * count
                bb[s, pl.ds(x, planes)] = INV_NOISE * (
                    total - count * fs[s, pl.ds(x + 1, planes), TOP : TOP + ny, :]
                )
            return _
        sweep(body, 0, lo, hi)

    me = (gx * gy_n + gy) * gz_n + gz
    lane_row = lax.broadcasted_iota(jnp.int32, (1, LANES), 1)

    def begin_sums(i, sums):
        row = jnp.zeros((1, LANES), jnp.float32)
        for n, share in enumerate(sums):
            total = jnp.sum(jnp.sum(share, axis=0, keepdims=True), axis=1, keepdims=True)
            row = jnp.where(lane_row == n, total, row)
        mine[i] = row
        rows_all[i, me] = row
        for offset in others:
            pltpu.make_async_remote_copy(
                src_ref=mine.at[i], dst_ref=rows_all.at[i, me], send_sem=sum_send,
                recv_sem=sum_recv.at[i], device_id=around(*offset), device_id_type=MESH,
            ).start()

    def end_sums(i):
        every = rows_all.at[i, pl.ds(0, len(others))]
        pltpu.make_async_copy(every, every, sum_recv.at[i]).wait()
        row = jnp.sum(rows_all[i], axis=0)
        pltpu.make_async_copy(every, every, sum_send).wait()
        return [
            jnp.sum(jnp.where(lane_row == n, row, 0.0), axis=1, keepdims=True) for n in range(2 * SETS)
        ]

    norm, size, alpha, beta = {}, {}, {}, {}

    def scalars(i):
        totals = end_sums(i)
        norm[i], product = totals[:SETS], totals[SETS:]
        if i == 0:
            size[i] = [n / d for n, d in zip(norm[i], product)]
        else:
            ratio = [n / w for n, w in zip(norm[i], norm[i - 1])]
            size[i] = [n / (d - b * n / a) for n, d, b, a in zip(norm[i], product, ratio, size[i - 1])]
            beta[i] = [jnp.broadcast_to(b, (8, LANES)) for b in ratio]
        alpha[i] = [jnp.broadcast_to(a, (8, LANES)) for a in size[i]]

    def advance(i):
        scalars(i)

        def body(x, sums):
            sums = list(sums)
            for s in range(SETS):
                for yb in range(yb_n):
                    at = (s, x, rows_of(yb), slice(None))
                    r, r_image = rr[at], ra[at]
                    p, p_image = r, r_image
                    q = fp[s, x + 1, inner_rows(yb), :]
                    q_image = ft[s, x + 1, inner_rows(yb), :]
                    if i > 0:
                        p = p + beta[i][s] * pp[at]
                        p_image = p_image + beta[i][s] * ap[at]
                        q = q + beta[i][s] * ss[at]
                        q_image = q_image + beta[i][s] * sa[at]
                    pp[at], ap[at] = p, p_image
                    if i + 2 < ITERS:
                        ss[at], sa[at] = q, q_image
                    xx[at] += alpha[i][s] * p
                    ax[at] += alpha[i][s] * p_image
                    r = r - alpha[i][s] * q
                    r_image = r_image - alpha[i][s] * q_image
                    rr[at], ra[at] = r, r_image
                    square = r * r
                    sums[s] = sums[s] + square
                    sums[SETS + s] = sums[SETS + s] + (r_image * r_image + ww[at] * square)
            return tuple(sums)
        begin_sums(i + 1, sweep(body, (zero,) * (2 * SETS), 0, nx, 2))

    no_faces = (zero,) * yb_n

    def sent(ys, s, x, yb, tile, acc):
        keep_rows(ys, s, x, yb, tile)
        acc = list(acc)
        acc[yb] = packed(acc[yb], s, x, tile)
        return tuple(acc)

    def send(kind, parts, acc):
        put_packed(parts[2], acc)
        copies = faces(kind, *parts)
        start(copies)
        return copies

    loads[0].wait()
    face_pass(fp, ysp, zsp)
    loads[2].wait()
    sweep(kappa, 0, 0, nx)
    for load in loads[1:2] + loads[3:]:
        load.wait()
    build(0)
    observe(0, 0, 2)
    pl.semaphore_wait(barrier, len(others))
    p_copies = faces(0, *p_kind)
    start(p_copies)

    def gap():
        build(1)
        observe(1, 0, 1)

    def emit_start(s, x, yb, out, acc):
        ft[s, x + 1, inner_rows(yb), :] = out
        ax[s, x, rows_of(yb), :] = out
        return sent(yst, s, x, yb, out, acc)

    t_copies = send(1, t_kind, apply(fp, p_copies, yrp, zrp, emit_start, no_faces, gap))
    s_copies = faces(2, *s_kind)

    def gap():
        face_pass(fs, yss, zss)
        start(s_copies)
        observe(1, 1, 2)

    def emit_residual(s, x, yb, out, acc):
        at = (s, x, rows_of(yb), slice(None))
        r = bb[at] - (out + ww[at] * xx[at])
        rr[at] = r
        fp[s, x + 1, inner_rows(yb), :] = r
        return sent(ysp, s, x, yb, r, acc)

    p_copies = send(0, p_kind, apply(ft, t_copies, yrt, zrt, emit_residual, no_faces, gap))

    def emit_state(s, x, yb, out, carry):
        ast[s, x, rows_of(yb), :] = out
        return carry

    def emit_first(s, x, yb, out, carry):
        at = (s, x, rows_of(yb), slice(None))
        ft[s, x + 1, inner_rows(yb), :] = out
        ra[at] = out
        acc, sums = carry[0], list(carry[1])
        square = rr[at] * rr[at]
        sums[s] = sums[s] + square
        sums[SETS + s] = sums[SETS + s] + (out * out + ww[at] * square)
        return (sent(yst, s, x, yb, out, acc), tuple(sums))

    acc, sums = apply(fp, p_copies, yrp, zrp, emit_first, (no_faces, (zero,) * (2 * SETS)))
    t_copies = send(1, t_kind, acc)
    begin_sums(0, sums)

    def emit_image(s, x, yb, out, acc):
        at = (s, x, rows_of(yb), slice(None))
        w = out + ww[at] * rr[at]
        fp[s, x + 1, inner_rows(yb), :] = w
        return sent(ysp, s, x, yb, w, acc)

    acc = apply(
        ft, t_copies, yrt, zrt, emit_image, no_faces,
        lambda: apply(fs, s_copies, yrs, zrs, emit_state, 0, part=ast),
    )
    p_copies = send(0, p_kind, acc)

    for i in range(ITERS - 1):
        last = i + 2 == ITERS

        def emit_inner(s, x, yb, out, acc):
            ft[s, x + 1, inner_rows(yb), :] = out
            return acc if last else sent(yst, s, x, yb, out, acc)

        def emit_outer(s, x, yb, out, acc):
            at = (s, x, rows_of(yb), slice(None))
            w = fp[s, x + 1, inner_rows(yb), :]
            z = out + ww[at] * w
            if i > 0:
                z = z + beta[i][s] * zz[at]
            if i + 3 < ITERS:
                zz[at] = z
            w = w - alpha[i][s] * z
            fp[s, x + 1, inner_rows(yb), :] = w
            return sent(ysp, s, x, yb, w, acc)

        acc = apply(fp, p_copies, yrp, zrp, emit_inner, no_faces)
        if last:
            advance(i)
        else:
            t_copies = send(1, t_kind, acc)
            acc = apply(
                ft, t_copies, yrt, zrt, emit_outer, no_faces, functools.partial(advance, i)
            )
            p_copies = send(0, p_kind, acc)

    i = ITERS - 1
    scalars(i)

    def finish(x, _):
        for yb in range(yb_n):
            total = zero
            for s in range(SETS):
                at = (s, x, rows_of(yb), slice(None))
                p = rr[at] + beta[i][s] * pp[at]
                p_image = ra[at] + beta[i][s] * ap[at]
                adjoint = xx[at] + alpha[i][s] * p
                image = ax[at] + alpha[i][s] * p_image
                adj_ref[at] = adjoint
                total = total + (adjoint * ast[at] + image * fs[s, x + 1, inner_rows(yb), :])
            grad_ref[x, rows_of(yb), :] = -2.0 * kap[x, rows_of(yb), :] * total
        return _
    sweep(finish, 0, 0, nx, 2)


def on_device(sizes, log_range, state, adjoint_start, obs_index, obs_value):
    nx, ny, nz = log_range.shape
    nobs = obs_index.shape[-1]
    f32 = jnp.float32
    field = pltpu.VMEM((SETS, nx, ny, nz), f32)
    padded = pltpu.VMEM((SETS, nx + 2, ny + 2 * TOP, nz), f32)
    yface = pltpu.VMEM((2, SETS, nx, nz), f32)
    zsent = pltpu.VMEM((ny, LANES), f32)
    zgot = pltpu.VMEM((2, ny, LANES), f32)
    vmem = pl.BlockSpec(memory_space=pltpu.VMEM)
    hbm = pl.BlockSpec(memory_space=pltpu.HBM)
    dma = pltpu.SemaphoreType.DMA
    return pl.pallas_call(
        functools.partial(kernel, sizes),
        out_shape=(
            jax.ShapeDtypeStruct((nx, ny, nz), f32),
            jax.ShapeDtypeStruct((SETS, nx, ny, nz), f32),
        ),
        in_specs=[hbm] * 5,
        out_specs=(vmem, vmem),
        scratch_shapes=[
            pltpu.VMEM((nx, ny, nz), f32),
            padded, padded, padded,
            field, field, field, field, field, field, field, field, field, field, field, field, field,
            yface, yface, yface, zsent, zsent, zsent, yface, yface, yface, zgot, zgot, zgot,
            pltpu.VMEM((6 * LANES, nobs), jnp.bfloat16),
            pltpu.VMEM((256, nobs), jnp.bfloat16),
            pltpu.VMEM((SETS, 1, nobs), jnp.int32),
            pltpu.VMEM((SETS, 1, nobs), f32),
            pltpu.VMEM((ITERS, sizes[0] * sizes[1] * sizes[2], 1, LANES), f32),
            pltpu.VMEM((ITERS, 1, LANES), f32),
            dma((3, 6)), dma((3, 6)), dma, dma((ITERS,)),
            dma((6,)),
        ],
        compiler_params=pltpu.CompilerParams(
            collective_id=0, has_side_effects=True, vmem_limit_bytes=60 * 1024 * 1024
        ),
    )(
        log_range, state, adjoint_start,
        obs_index.reshape(SETS, 1, nobs), obs_value.reshape(SETS, 1, nobs),
    )


def solution(mesh):
    sizes = (mesh.shape["gx"], mesh.shape["gy"], mesh.shape["gz"])
    whole, per_set = P("gx", "gy", "gz"), P(None, "gx", "gy", "gz")
    obs = P(None, "gx", "gy", "gz", None)
    return jax.shard_map(
        functools.partial(on_device, sizes), mesh=mesh,
        in_specs=(whole, per_set, per_set, obs, obs), out_specs=(whole, per_set), check_vma=False,
    )
```

```python
import functools

import jax
import jax.numpy as jnp
from jax import lax
from jax.experimental import pallas as pl
from jax.experimental.pallas import tpu as pltpu
from jax.sharding import PartitionSpec as P

ITERS = 4
SETS = 2
LANES = 128
TOP = 8
MESH = pl.DeviceIdType.MESH
INTERIOR = 15
WHOLE = 16
INV_NOISE = 4.0


def kernel(
    sizes,
    lr_hbm, st_hbm, x0_hbm, index_hbm, value_hbm,
    grad_ref, adj_ref,
    kap, fp, ft, fs, part, xx, ax, pp, ap, ss, sa, rr, ra, rs, rt, zz, ww, bb, ast,
    ysp, yst, yss, zsp, zst, zss, yrp, yrt, yrs, zrp, zrt, zrs,
    onehot_lo, onehot_hi, index_ref, value_ref, rows_all, rows_near, mine, ours,
    send_sem, recv_sem, sum_send, sum_recv, local_sem, out_sem,
):
    gx_n, gy_n, gz_n = sizes
    nx, ny = kap.shape[0], kap.shape[1]
    yb_n = ny // 8
    gx, gy, gz = lax.axis_index("gx"), lax.axis_index("gy"), lax.axis_index("gz")

    def around(dx, dy, dz):
        return (
            lax.rem(gx + dx + gx_n, gx_n),
            lax.rem(gy + dy + gy_n, gy_n),
            lax.rem(gz + dz + gz_n, gz_n),
        )

    def length(offset):
        return sum(min(d, n - d) for d, n in zip(offset, sizes))

    others = [
        (dx, dy, dz) for dx in range(gx_n) for dy in range(gy_n) for dz in range(gz_n)
    ][1:]
    others.sort(key=length, reverse=True)

    inner = (slice(None), pl.ds(1, nx), pl.ds(TOP, ny), slice(None))
    loads = [
        pltpu.make_async_copy(x0_hbm, fp.at[inner], local_sem.at[0]),
        pltpu.make_async_copy(st_hbm, fs.at[inner], local_sem.at[1]),
        pltpu.make_async_copy(lr_hbm, kap, local_sem.at[2]),
        pltpu.make_async_copy(x0_hbm, xx, local_sem.at[3]),
        pltpu.make_async_copy(index_hbm, index_ref, local_sem.at[4]),
        pltpu.make_async_copy(value_hbm, value_ref, local_sem.at[5]),
    ]
    for load in loads:
        load.start()

    barrier = pltpu.get_barrier_semaphore()
    for offset in others:
        pl.semaphore_signal(barrier, inc=1, device_id=around(*offset), device_id_type=MESH)

    lane = lax.broadcasted_iota(jnp.int32, (8, LANES), 1)
    sub = lax.broadcasted_iota(jnp.int32, (8, LANES), 0)
    pair = lane // 2
    even = lane % 2 == 0
    zero = jnp.zeros((8, LANES), jnp.float32)

    def faces(kind, field, ys, zs, yr, zr):
        moves = [
            (field.at[:, nx, pl.ds(TOP, ny), :], field.at[:, 0, pl.ds(TOP, ny), :], (1, 0, 0)),
            (field.at[:, 1, pl.ds(TOP, ny), :], field.at[:, nx + 1, pl.ds(TOP, ny), :], (-1, 0, 0)),
            (ys.at[1], yr.at[0], (0, 1, 0)),
            (ys.at[0], yr.at[1], (0, -1, 0)),
            (zs, zr.at[0], (0, 0, 1)),
            (zs, zr.at[1], (0, 0, -1)),
        ]
        return [
            pltpu.make_async_remote_copy(
                src_ref=src, dst_ref=dst, send_sem=send_sem.at[kind, k], recv_sem=recv_sem.at[kind, k],
                device_id=around(*offset), device_id_type=MESH,
            )
            for k, (src, dst, offset) in enumerate(moves)
        ]

    def start(copies):
        for k in (4, 5, 2, 3, 0, 1):
            copies[k].start()

    def keep_rows(ys, s, x, yb, tile):
        if yb == 0:
            ys[0, s, pl.ds(x, 1), :] = tile[0:1, :]
        if yb == yb_n - 1:
            ys[1, s, pl.ds(x, 1), :] = tile[7:8, :]

    def packed(acc, s, x, tile):
        j = s * nx + x
        return jnp.where(pair == j, pltpu.roll(tile, 2 * j + 1, 1), acc)

    def put_packed(zs, acc):
        for yb in range(yb_n):
            zs[8 * yb : 8 * yb + 8, :] = acc[yb]

    def sweep(body, carry, lo, hi, unroll=1):
        def several(n, carry):
            for k in range(unroll):
                carry = body(lo + n * unroll + k, carry)
            return carry
        return lax.fori_loop(0, (hi - lo) // unroll, several, carry)

    def face_pass(field, ys, zs):
        def body(x, acc):
            acc = list(acc)
            for s in range(SETS):
                for yb in range(yb_n):
                    tile = field[s, x + 1, TOP + 8 * yb : TOP + 8 * yb + 8, :]
                    keep_rows(ys, s, x, yb, tile)
                    acc[yb] = packed(acc[yb], s, x, tile)
            return tuple(acc)
        put_packed(zs, sweep(body, (zero,) * yb_n, 0, nx, WHOLE))

    def rows_of(yb):
        return slice(8 * yb, 8 * yb + 8)

    def inner_rows(yb):
        return slice(TOP + 8 * yb, TOP + 8 * yb + 8)

    sides = (lane == 0) | (lane == LANES - 1)

    def apply(field, copies, yr, zr, emit, carry, gap=None, mid=None, part=part):
        def partial(x, _, lower=True, upper=True):
            for s in range(SETS):
                for yb in range(yb_n):
                    r = TOP + 8 * yb
                    c = field[s, x + 1, r : r + 8, :]
                    ym = field[s, x + 1, r - 1 : r + 7, :]
                    yp = field[s, x + 1, r + 1 : r + 9, :]
                    if yb == 0:
                        ym = jnp.where(sub == 0, 0.0, ym)
                    if yb == yb_n - 1:
                        yp = jnp.where(sub == 7, 0.0, yp)
                    zm = jnp.where(lane == 0, 0.0, pltpu.roll(c, 1, 1))
                    zp = jnp.where(lane == LANES - 1, 0.0, pltpu.roll(c, LANES - 1, 1))
                    beside = (ym + yp) + (zm + zp)
                    if lower:
                        beside = beside + field[s, x, r : r + 8, :]
                    if upper:
                        beside = beside + field[s, x + 2, r : r + 8, :]
                    part[s, x, rows_of(yb), :] = (kap[x, rows_of(yb), :] + 6.0) * c - beside
            return _

        partial(0, 0, lower=False)
        partial(nx - 1, 0, upper=False)
        sweep(partial, 0, 1, nx - 1, INTERIOR)
        if gap is not None:
            gap()
        for k in (2, 3, 4, 5):
            copies[k].wait_recv()
        zc = [
            jnp.where(even, zr[0, rows_of(yb), :], pltpu.roll(zr[1, rows_of(yb), :], LANES - 2, 1))
            for yb in range(yb_n)
        ]

        def complete(x, carry, slab=None):
            for s in range(SETS):
                shift = lax.rem(LANES - 2 * (s * nx + x), LANES)
                for yb in range(yb_n):
                    out = part[s, x, rows_of(yb), :]
                    out = out - jnp.where(sides, pltpu.roll(zc[yb], shift, 1), 0.0)
                    if yb == 0:
                        out = out - jnp.where(sub == 0, yr[0, s, pl.ds(x, 1), :], 0.0)
                    if yb == yb_n - 1:
                        out = out - jnp.where(sub == 7, yr[1, s, pl.ds(x, 1), :], 0.0)
                    if slab is not None:
                        out = out - field[s, slab, inner_rows(yb), :]
                    carry = emit(s, x, yb, out, carry)
            return carry

        carry = sweep(complete, carry, 1, nx - 1, INTERIOR)
        if mid is not None:
            mid()
        for k in (0, 1):
            copies[k].wait_recv()
        carry = complete(0, carry, 0)
        carry = complete(nx - 1, carry, nx + 1)
        for copy in copies:
            copy.wait_send()
        return carry

    p_kind = (fp, ysp, zsp, yrp, zrp)
    t_kind = (ft, yst, zst, yrt, zrt)
    s_kind = (fs, yss, zss, yrs, zrs)

    def kappa(x, _):
        kap[x] = 4.0 * jnp.exp(-2.0 * kap[x])
        return _

    nobs = index_ref.shape[2]
    rows = onehot_hi.shape[0]
    step = 512
    bf16 = jnp.bfloat16
    planes = rows // ny

    halves = 2
    rows_half = nx * ny // halves

    def spread(count, numbers, weights):
        hit = lax.broadcasted_iota(jnp.int32, (count, step), 0).astype(bf16) == numbers.astype(
            jnp.float32
        ).astype(bf16)
        return [jnp.where(hit, weight, jnp.zeros_like(weight)) for weight in weights]

    def build(s):
        for k in range(0, nobs, step):
            cell = index_ref[s, :, k : k + step]
            low = cell % LANES + cell // (rows_half * LANES) * LANES
            v = value_ref[s, :, k : k + step]
            v1 = v.astype(bf16)
            v2 = (v - v1.astype(jnp.float32)).astype(bf16)
            for n, tile in enumerate(spread(halves * LANES, low, (jnp.ones_like(v1), v1, v2))):
                onehot_lo[halves * LANES * n : halves * LANES * (n + 1), k : k + step] = tile

    def observe(s, lo, hi):
        def body(m, _):
            for k in range(0, nobs, step):
                high = index_ref[s, :, k : k + step] // LANES % rows_half
                for r in range(0, rows, 256):
                    ones = jnp.ones((1, step), bf16)
                    onehot_hi[r : r + 256, k : k + step] = spread(256, high - (m * rows + r), (ones,))[0]
            sums = lax.dot_general(
                onehot_hi[...], onehot_lo[...], (((1,), (1,)), ((), ())),
                preferred_element_type=jnp.float32,
            )
            for h in range(halves):
                count, high, low = (
                    sums[:, (halves * n + h) * LANES : (halves * n + h + 1) * LANES] for n in range(3)
                )
                count = count.reshape(planes, ny, LANES)
                total = (high + low).reshape(planes, ny, LANES)
                x = h * (nx // halves) + m * planes
                ww[s, pl.ds(x, planes)] = INV_NOISE * count
                bb[s, pl.ds(x, planes)] = INV_NOISE * (
                    total - count * fs[s, pl.ds(x + 1, planes), TOP : TOP + ny, :]
                )
            return _
        sweep(body, 0, lo, hi)

    me = (gx * gy_n + gy) * gz_n + gz
    lane_row = lax.broadcasted_iota(jnp.int32, (1, LANES), 1)

    def row_copies(i, source, to, slot, sent, got, offsets):
        for offset in offsets:
            pltpu.make_async_remote_copy(
                src_ref=source.at[i], dst_ref=to.at[i, slot], send_sem=sent,
                recv_sem=got, device_id=around(*offset), device_id_type=MESH,
            ).start()

    def wait_rows(i, rows, count, sem):
        every = rows.at[i, pl.ds(0, count)]
        pltpu.make_async_copy(every, every, sem).wait()

    near = [(0, 0, dz) for dz in range(1, gz_n)]
    far = [offset for offset in others if offset[2] == 0]
    direct = ITERS - 1

    def begin_sums(i, sums):
        row = jnp.zeros((1, LANES), jnp.float32)
        for n, share in enumerate(sums):
            total = jnp.sum(jnp.sum(share, axis=0, keepdims=True), axis=1, keepdims=True)
            row = jnp.where(lane_row == n, total, row)
        mine[i] = row
        if i == direct:
            rows_all[i, me] = row
            row_copies(i, mine, rows_all, me, sum_send.at[0], sum_recv.at[i, 0], others)
        else:
            rows_near[i, gz] = row
            row_copies(i, mine, rows_near, gz, sum_send.at[0], sum_recv.at[i, 0], near)

    def forward_sums(i):
        wait_rows(i, rows_near, len(near), sum_recv.at[i, 0])
        row = jnp.sum(rows_near[i], axis=0)
        group = gx * gy_n + gy
        ours[i] = row
        rows_all[i, group] = row
        row_copies(i, ours, rows_all, group, sum_send.at[1], sum_recv.at[i, 1], far)

    def end_sums(i):
        if i == direct:
            wait_rows(i, rows_all, len(others), sum_recv.at[i, 0])
            row = jnp.sum(rows_all[i], axis=0)
            wait_rows(i, rows_all, len(others), sum_send.at[0])
        else:
            wait_rows(i, rows_all, len(far), sum_recv.at[i, 1])
            row = jnp.sum(rows_all[i, 0 : gx_n * gy_n], axis=0)
            wait_rows(i, rows_near, len(near), sum_send.at[0])
            wait_rows(i, rows_all, len(far), sum_send.at[1])
        return [
            jnp.sum(jnp.where(lane_row == n, row, 0.0), axis=1, keepdims=True) for n in range(2 * SETS)
        ]

    norm, size, alpha, beta = {}, {}, {}, {}

    def scalars(i):
        totals = end_sums(i)
        norm[i], product = totals[:SETS], totals[SETS:]
        if i == 0:
            size[i] = [n / d for n, d in zip(norm[i], product)]
        else:
            ratio = [n / w for n, w in zip(norm[i], norm[i - 1])]
            size[i] = [n / (d - b * n / a) for n, d, b, a in zip(norm[i], product, ratio, size[i - 1])]
            beta[i] = [jnp.broadcast_to(b, (8, LANES)) for b in ratio]
        alpha[i] = [jnp.broadcast_to(a, (8, LANES)) for a in size[i]]

    def advance(i):
        scalars(i)

        def body(x, sums):
            sums = list(sums)
            for s in range(SETS):
                for yb in range(yb_n):
                    at = (s, x, rows_of(yb), slice(None))
                    q = fp[s, x + 1, inner_rows(yb), :]
                    q_image = ft[s, x + 1, inner_rows(yb), :]
                    if i > 0:
                        q = q + beta[i][s] * ss[at]
                        q_image = q_image + beta[i][s] * sa[at]
                    if i + 2 < ITERS:
                        ss[at], sa[at] = q, q_image
                    fresh, fresh_image = (rr, ra) if i % 2 else (rs, rt)
                    old, old_image = (rs, rt) if i % 2 else (rr, ra)
                    r = old[at] - alpha[i][s] * q
                    r_image = old_image[at] - alpha[i][s] * q_image
                    fresh[at], fresh_image[at] = r, r_image
                    square = r * r
                    sums[s] = sums[s] + square
                    sums[SETS + s] = sums[SETS + s] + (r_image * r_image + ww[at] * square)
            return tuple(sums)
        begin_sums(i + 1, sweep(body, (zero,) * (2 * SETS), 0, nx, 4))

        def settle(x, _):
            old, old_image = (rs, rt) if i % 2 else (rr, ra)
            for s in range(SETS):
                for yb in range(yb_n):
                    at = (s, x, rows_of(yb), slice(None))
                    p, p_image = old[at], old_image[at]
                    if i > 0:
                        p = p + beta[i][s] * pp[at]
                        p_image = p_image + beta[i][s] * ap[at]
                    pp[at], ap[at] = p, p_image
                    xx[at] += alpha[i][s] * p
                    ax[at] += alpha[i][s] * p_image
            return _
        sweep(settle, 0, 0, nx, 4)

    no_faces = (zero,) * yb_n

    def sent(ys, s, x, yb, tile, acc):
        keep_rows(ys, s, x, yb, tile)
        acc = list(acc)
        acc[yb] = packed(acc[yb], s, x, tile)
        return tuple(acc)

    def send(kind, parts, acc):
        put_packed(parts[2], acc)
        copies = faces(kind, *parts)
        start(copies)
        return copies

    loads[0].wait()
    face_pass(fp, ysp, zsp)
    loads[2].wait()
    sweep(kappa, 0, 0, nx)
    for load in loads[1:2] + loads[3:]:
        load.wait()
    build(0)
    observe(0, 0, 2)
    pl.semaphore_wait(barrier, len(others))
    p_copies = faces(0, *p_kind)
    start(p_copies)

    def gap():
        build(1)
        observe(1, 0, 2)

    def emit_start(s, x, yb, out, acc):
        ft[s, x + 1, inner_rows(yb), :] = out
        ax[s, x, rows_of(yb), :] = out
        return sent(yst, s, x, yb, out, acc)

    t_copies = send(1, t_kind, apply(fp, p_copies, yrp, zrp, emit_start, no_faces, gap))
    s_copies = faces(2, *s_kind)

    def gap():
        face_pass(fs, yss, zss)
        start(s_copies)

    def emit_residual(s, x, yb, out, acc):
        at = (s, x, rows_of(yb), slice(None))
        r = bb[at] - (out + ww[at] * xx[at])
        rr[at] = r
        fp[s, x + 1, inner_rows(yb), :] = r
        return sent(ysp, s, x, yb, r, acc)

    p_copies = send(0, p_kind, apply(ft, t_copies, yrt, zrt, emit_residual, no_faces, gap))

    def emit_state(s, x, yb, out, carry):
        ast[s, x, rows_of(yb), :] = out
        return carry

    def emit_first(s, x, yb, out, carry):
        at = (s, x, rows_of(yb), slice(None))
        ft[s, x + 1, inner_rows(yb), :] = out
        ra[at] = out
        acc, sums = carry[0], list(carry[1])
        square = rr[at] * rr[at]
        sums[s] = sums[s] + square
        sums[SETS + s] = sums[SETS + s] + (out * out + ww[at] * square)
        return (sent(yst, s, x, yb, out, acc), tuple(sums))

    acc, sums = apply(fp, p_copies, yrp, zrp, emit_first, (no_faces, (zero,) * (2 * SETS)))
    t_copies = send(1, t_kind, acc)
    begin_sums(0, sums)

    def emit_image(s, x, yb, out, acc):
        at = (s, x, rows_of(yb), slice(None))
        w = out + ww[at] * rr[at]
        fp[s, x + 1, inner_rows(yb), :] = w
        return sent(ysp, s, x, yb, w, acc)

    acc = apply(
        ft, t_copies, yrt, zrt, emit_image, no_faces,
        lambda: apply(fs, s_copies, yrs, zrs, emit_state, 0, part=ast), lambda: forward_sums(0),
    )
    p_copies = send(0, p_kind, acc)

    for i in range(ITERS - 1):
        last = i + 2 == ITERS

        def emit_inner(s, x, yb, out, acc):
            ft[s, x + 1, inner_rows(yb), :] = out
            return acc if last else sent(yst, s, x, yb, out, acc)

        def emit_outer(s, x, yb, out, acc):
            at = (s, x, rows_of(yb), slice(None))
            w = fp[s, x + 1, inner_rows(yb), :]
            z = out + ww[at] * w
            if i > 0:
                z = z + beta[i][s] * zz[at]
            if i + 3 < ITERS:
                zz[at] = z
            w = w - alpha[i][s] * z
            fp[s, x + 1, inner_rows(yb), :] = w
            return sent(ysp, s, x, yb, w, acc)

        acc = apply(fp, p_copies, yrp, zrp, emit_inner, no_faces)
        if last:
            advance(i)
        else:
            t_copies = send(1, t_kind, acc)
            acc = apply(
                ft, t_copies, yrt, zrt, emit_outer, no_faces, functools.partial(advance, i),
                functools.partial(forward_sums, i + 1),
            )
            p_copies = send(0, p_kind, acc)

    i = ITERS - 1
    scalars(i)

    final, final_image = (rr, ra) if (ITERS - 2) % 2 else (rs, rt)

    def finish(x, _):
        for yb in range(yb_n):
            total = zero
            for s in range(SETS):
                at = (s, x, rows_of(yb), slice(None))
                p = final[at] + beta[i][s] * pp[at]
                p_image = final_image[at] + beta[i][s] * ap[at]
                adjoint = xx[at] + alpha[i][s] * p
                image = ax[at] + alpha[i][s] * p_image
                xx[at] = adjoint
                total = total + (adjoint * ast[at] + image * fs[s, x + 1, inner_rows(yb), :])
            kap[x, rows_of(yb), :] = -2.0 * kap[x, rows_of(yb), :] * total
        return _

    stores = []
    share = nx // 4
    for n in range(4):
        sweep(finish, 0, n * share, (n + 1) * share, 2)
        at = pl.ds(n * share, share)
        stores.append(pltpu.make_async_copy(xx.at[:, at], adj_ref.at[:, at], out_sem.at[n, 0]))
        stores.append(pltpu.make_async_copy(kap.at[at], grad_ref.at[at], out_sem.at[n, 1]))
        stores[-2].start()
        stores[-1].start()
    for store in stores:
        store.wait()


def hand_over(gradient, adjoint):
    nx, ny, nz = gradient.shape
    share = nx // 4

    def body(gradient_hbm, adjoint_hbm, gradient_out, adjoint_out, gradient_buf, adjoint_buf, got, put):
        reads, writes = [], []
        for n in range(4):
            at = pl.ds(n * share, share)
            reads += [
                pltpu.make_async_copy(gradient_hbm.at[at], gradient_buf.at[at], got.at[n, 0]),
                pltpu.make_async_copy(adjoint_hbm.at[:, at], adjoint_buf.at[:, at], got.at[n, 1]),
            ]
            writes += [
                pltpu.make_async_copy(gradient_buf.at[at], gradient_out.at[at], put.at[n, 0]),
                pltpu.make_async_copy(adjoint_buf.at[:, at], adjoint_out.at[:, at], put.at[n, 1]),
            ]
        for read in reads:
            read.start()
        for read, write in zip(reads, writes):
            read.wait()
            write.start()
        for write in writes:
            write.wait()

    hbm = pl.BlockSpec(memory_space=pl.ANY)
    return pl.pallas_call(
        body,
        out_shape=(
            jax.ShapeDtypeStruct(gradient.shape, gradient.dtype),
            jax.ShapeDtypeStruct(adjoint.shape, adjoint.dtype),
        ),
        in_specs=[hbm, hbm], out_specs=(hbm, hbm),
        scratch_shapes=[
            pltpu.VMEM(gradient.shape, gradient.dtype), pltpu.VMEM(adjoint.shape, adjoint.dtype),
            pltpu.SemaphoreType.DMA((4, 2)), pltpu.SemaphoreType.DMA((4, 2)),
        ],
        compiler_params=pltpu.CompilerParams(vmem_limit_bytes=60 * 1024 * 1024),
    )(gradient, adjoint)


def on_device(sizes, log_range, state, adjoint_start, obs_index, obs_value):
    nx, ny, nz = log_range.shape
    nobs = obs_index.shape[-1]
    f32 = jnp.float32
    field = pltpu.VMEM((SETS, nx, ny, nz), f32)
    padded = pltpu.VMEM((SETS, nx + 2, ny + 2 * TOP, nz), f32)
    yface = pltpu.VMEM((2, SETS, nx, nz), f32)
    zsent = pltpu.VMEM((ny, LANES), f32)
    zgot = pltpu.VMEM((2, ny, LANES), f32)
    hbm = pl.BlockSpec(memory_space=pl.ANY)
    dma = pltpu.SemaphoreType.DMA
    gradient, adjoint = pl.pallas_call(
        functools.partial(kernel, sizes),
        out_shape=(
            jax.ShapeDtypeStruct((nx, ny, nz), f32),
            jax.ShapeDtypeStruct((SETS, nx, ny, nz), f32),
        ),
        in_specs=[hbm] * 5,
        out_specs=(hbm, hbm),
        scratch_shapes=[
            pltpu.VMEM((nx, ny, nz), f32),
            padded, padded, padded, field, field,
            field, field, field, field, field, field, field, field, field, field, field, field, field,
            yface, yface, yface, zsent, zsent, zsent, yface, yface, yface, zgot, zgot, zgot,
            pltpu.VMEM((6 * LANES, nobs), jnp.bfloat16),
            pltpu.VMEM((256, nobs), jnp.bfloat16),
            pltpu.VMEM((SETS, 1, nobs), jnp.int32),
            pltpu.VMEM((SETS, 1, nobs), f32),
            pltpu.VMEM((ITERS, sizes[0] * sizes[1] * sizes[2], 1, LANES), f32),
            pltpu.VMEM((ITERS, sizes[2], 1, LANES), f32),
            pltpu.VMEM((ITERS, 1, LANES), f32),
            pltpu.VMEM((ITERS, 1, LANES), f32),
            dma((3, 6)), dma((3, 6)), dma((2,)), dma((ITERS, 2)),
            dma((6,)), dma((4, 2)),
        ],
        compiler_params=pltpu.CompilerParams(
            collective_id=0, has_side_effects=True, vmem_limit_bytes=60 * 1024 * 1024
        ),
    )(
        log_range, state, adjoint_start,
        obs_index.reshape(SETS, 1, nobs), obs_value.reshape(SETS, 1, nobs),
    )
    return hand_over(gradient, adjoint)


def solution(mesh):
    sizes = (mesh.shape["gx"], mesh.shape["gy"], mesh.shape["gz"])
    whole, per_set = P("gx", "gy", "gz"), P(None, "gx", "gy", "gz")
    obs = P(None, "gx", "gy", "gz", None)
    return jax.shard_map(
        functools.partial(on_device, sizes), mesh=mesh,
        in_specs=(whole, per_set, per_set, obs, obs), out_specs=(whole, per_set), check_vma=False,
    )
```

```python
import functools

import jax
import jax.numpy as jnp
from jax import lax
from jax.experimental import pallas as pl
from jax.experimental.pallas import tpu as pltpu
from jax.sharding import PartitionSpec as P

ITERS = 4
SETS = 2
LANES = 128
TOP = 8
MESH = pl.DeviceIdType.MESH
INTERIOR = 15
WHOLE = 16
INV_NOISE = 4.0


def kernel(
    sizes,
    lr_hbm, st_hbm, x0_hbm, index_hbm, value_hbm,
    grad_ref, adj_ref,
    kap, fp, ft, fs, part, xx, ax, pp, ap, ss, sa, rr, ra, rs, rt, zz, ww, bb, ast,
    ysp, yst, yss, zsp, zst, zss, yrp, yrt, yrs, zrp, zrt, zrs,
    onehot_lo, onehot_hi, index_ref, value_ref, rows_all, rows_near, mine, ours,
    send_sem, recv_sem, sum_send, sum_recv, local_sem, out_sem,
):
    gx_n, gy_n, gz_n = sizes
    nx, ny = kap.shape[0], kap.shape[1]
    yb_n = ny // 8
    gx, gy, gz = lax.axis_index("gx"), lax.axis_index("gy"), lax.axis_index("gz")

    def around(dx, dy, dz):
        return (
            lax.rem(gx + dx + gx_n, gx_n),
            lax.rem(gy + dy + gy_n, gy_n),
            lax.rem(gz + dz + gz_n, gz_n),
        )

    def length(offset):
        return sum(min(d, n - d) for d, n in zip(offset, sizes))

    others = [
        (dx, dy, dz) for dx in range(gx_n) for dy in range(gy_n) for dz in range(gz_n)
    ][1:]
    others.sort(key=length, reverse=True)

    inner = (slice(None), pl.ds(1, nx), pl.ds(TOP, ny), slice(None))
    loads = [
        pltpu.make_async_copy(x0_hbm, fp.at[inner], local_sem.at[0]),
        pltpu.make_async_copy(st_hbm, fs.at[inner], local_sem.at[1]),
        pltpu.make_async_copy(lr_hbm, kap, local_sem.at[2]),
        pltpu.make_async_copy(x0_hbm, xx, local_sem.at[3]),
        pltpu.make_async_copy(index_hbm, index_ref, local_sem.at[4]),
        pltpu.make_async_copy(value_hbm, value_ref, local_sem.at[5]),
    ]
    for load in loads:
        load.start()

    barrier = pltpu.get_barrier_semaphore()
    for offset in others:
        pl.semaphore_signal(barrier, inc=1, device_id=around(*offset), device_id_type=MESH)

    lane = lax.broadcasted_iota(jnp.int32, (8, LANES), 1)
    sub = lax.broadcasted_iota(jnp.int32, (8, LANES), 0)
    pair = lane // 2
    even = lane % 2 == 0
    zero = jnp.zeros((8, LANES), jnp.float32)

    def faces(kind, field, ys, zs, yr, zr):
        moves = [
            (field.at[:, nx, pl.ds(TOP, ny), :], field.at[:, 0, pl.ds(TOP, ny), :], (1, 0, 0)),
            (field.at[:, 1, pl.ds(TOP, ny), :], field.at[:, nx + 1, pl.ds(TOP, ny), :], (-1, 0, 0)),
            (ys.at[1], yr.at[0], (0, 1, 0)),
            (ys.at[0], yr.at[1], (0, -1, 0)),
            (zs, zr.at[0], (0, 0, 1)),
            (zs, zr.at[1], (0, 0, -1)),
        ]
        return [
            pltpu.make_async_remote_copy(
                src_ref=src, dst_ref=dst, send_sem=send_sem.at[kind, k], recv_sem=recv_sem.at[kind, k],
                device_id=around(*offset), device_id_type=MESH,
            )
            for k, (src, dst, offset) in enumerate(moves)
        ]

    def start(copies):
        for k in (4, 5, 2, 3, 0, 1):
            copies[k].start()

    def keep_rows(ys, s, x, yb, tile):
        if yb == 0:
            ys[0, s, pl.ds(x, 1), :] = tile[0:1, :]
        if yb == yb_n - 1:
            ys[1, s, pl.ds(x, 1), :] = tile[7:8, :]

    def packed(acc, s, x, tile):
        j = s * nx + x
        return jnp.where(pair == j, pltpu.roll(tile, 2 * j + 1, 1), acc)

    def put_packed(zs, acc):
        for yb in range(yb_n):
            zs[8 * yb : 8 * yb + 8, :] = acc[yb]

    def sweep(body, carry, lo, hi, unroll=1):
        def several(n, carry):
            for k in range(unroll):
                carry = body(lo + n * unroll + k, carry)
            return carry
        return lax.fori_loop(0, (hi - lo) // unroll, several, carry)

    def face_pass(field, ys, zs):
        def body(x, acc):
            acc = list(acc)
            for s in range(SETS):
                for yb in range(yb_n):
                    tile = field[s, x + 1, TOP + 8 * yb : TOP + 8 * yb + 8, :]
                    keep_rows(ys, s, x, yb, tile)
                    acc[yb] = packed(acc[yb], s, x, tile)
            return tuple(acc)
        put_packed(zs, sweep(body, (zero,) * yb_n, 0, nx, WHOLE))

    def rows_of(yb):
        return slice(8 * yb, 8 * yb + 8)

    def inner_rows(yb):
        return slice(TOP + 8 * yb, TOP + 8 * yb + 8)

    sides = (lane == 0) | (lane == LANES - 1)

    def apply(field, copies, yr, zr, emit, carry, gap=None, mid=None, part=part):
        def partial(x, _, lower=True, upper=True):
            for s in range(SETS):
                for yb in range(yb_n):
                    r = TOP + 8 * yb
                    c = field[s, x + 1, r : r + 8, :]
                    ym = field[s, x + 1, r - 1 : r + 7, :]
                    yp = field[s, x + 1, r + 1 : r + 9, :]
                    if yb == 0:
                        ym = jnp.where(sub == 0, 0.0, ym)
                    if yb == yb_n - 1:
                        yp = jnp.where(sub == 7, 0.0, yp)
                    zm = jnp.where(lane == 0, 0.0, pltpu.roll(c, 1, 1))
                    zp = jnp.where(lane == LANES - 1, 0.0, pltpu.roll(c, LANES - 1, 1))
                    beside = (ym + yp) + (zm + zp)
                    if lower:
                        beside = beside + field[s, x, r : r + 8, :]
                    if upper:
                        beside = beside + field[s, x + 2, r : r + 8, :]
                    part[s, x, rows_of(yb), :] = (kap[x, rows_of(yb), :] + 6.0) * c - beside
            return _

        partial(0, 0, lower=False)
        partial(nx - 1, 0, upper=False)
        sweep(partial, 0, 1, nx - 1, INTERIOR)
        if gap is not None:
            gap()
        for k in (2, 3, 4, 5):
            copies[k].wait_recv()
        zc = [
            jnp.where(even, zr[0, rows_of(yb), :], pltpu.roll(zr[1, rows_of(yb), :], LANES - 2, 1))
            for yb in range(yb_n)
        ]

        def complete(x, carry, slab=None):
            for s in range(SETS):
                shift = lax.rem(LANES - 2 * (s * nx + x), LANES)
                for yb in range(yb_n):
                    out = part[s, x, rows_of(yb), :]
                    out = out - jnp.where(sides, pltpu.roll(zc[yb], shift, 1), 0.0)
                    if yb == 0:
                        out = out - jnp.where(sub == 0, yr[0, s, pl.ds(x, 1), :], 0.0)
                    if yb == yb_n - 1:
                        out = out - jnp.where(sub == 7, yr[1, s, pl.ds(x, 1), :], 0.0)
                    if slab is not None:
                        out = out - field[s, slab, inner_rows(yb), :]
                    carry = emit(s, x, yb, out, carry)
            return carry

        carry = sweep(complete, carry, 1, nx - 1, INTERIOR)
        if mid is not None:
            mid()
        for k in (0, 1):
            copies[k].wait_recv()
        carry = complete(0, carry, 0)
        carry = complete(nx - 1, carry, nx + 1)
        for copy in copies:
            copy.wait_send()
        return carry

    p_kind = (fp, ysp, zsp, yrp, zrp)
    t_kind = (ft, yst, zst, yrt, zrt)
    s_kind = (fs, yss, zss, yrs, zrs)

    def kappa(x, _):
        kap[x] = 4.0 * jnp.exp(-2.0 * kap[x])
        return _

    nobs = index_ref.shape[2]
    rows = onehot_hi.shape[0]
    step = 512
    bf16 = jnp.bfloat16
    planes = rows // ny

    halves = 2
    rows_half = nx * ny // halves

    def spread(count, numbers, weights):
        hit = lax.broadcasted_iota(jnp.int32, (count, step), 0).astype(bf16) == numbers.astype(
            jnp.float32
        ).astype(bf16)
        return [jnp.where(hit, weight, jnp.zeros_like(weight)) for weight in weights]

    def build(s):
        for k in range(0, nobs, step):
            cell = index_ref[s, :, k : k + step]
            low = cell % LANES + cell // (rows_half * LANES) * LANES
            v = value_ref[s, :, k : k + step]
            v1 = v.astype(bf16)
            v2 = (v - v1.astype(jnp.float32)).astype(bf16)
            for n, tile in enumerate(spread(halves * LANES, low, (jnp.ones_like(v1), v1, v2))):
                onehot_lo[halves * LANES * n : halves * LANES * (n + 1), k : k + step] = tile

    def observe(s, lo, hi):
        def body(m, _):
            for k in range(0, nobs, step):
                high = index_ref[s, :, k : k + step] // LANES % rows_half
                for r in range(0, rows, 256):
                    ones = jnp.ones((1, step), bf16)
                    onehot_hi[r : r + 256, k : k + step] = spread(256, high - (m * rows + r), (ones,))[0]
            sums = lax.dot_general(
                onehot_hi[...], onehot_lo[...], (((1,), (1,)), ((), ())),
                preferred_element_type=jnp.float32,
            )
            for h in range(halves):
                count, high, low = (
                    sums[:, (halves * n + h) * LANES : (halves * n + h + 1) * LANES] for n in range(3)
                )
                count = count.reshape(planes, ny, LANES)
                total = (high + low).reshape(planes, ny, LANES)
                x = h * (nx // halves) + m * planes
                ww[s, pl.ds(x, planes)] = INV_NOISE * count
                bb[s, pl.ds(x, planes)] = INV_NOISE * (
                    total - count * fs[s, pl.ds(x + 1, planes), TOP : TOP + ny, :]
                )
            return _
        sweep(body, 0, lo, hi)

    me = (gx * gy_n + gy) * gz_n + gz
    lane_row = lax.broadcasted_iota(jnp.int32, (1, LANES), 1)

    def row_copies(i, source, to, slot, sent, got, offsets):
        for offset in offsets:
            pltpu.make_async_remote_copy(
                src_ref=source.at[i], dst_ref=to.at[i, slot], send_sem=sent,
                recv_sem=got, device_id=around(*offset), device_id_type=MESH,
            ).start()

    def wait_rows(i, rows, count, sem):
        every = rows.at[i, pl.ds(0, count)]
        pltpu.make_async_copy(every, every, sem).wait()

    near = [(0, 0, dz) for dz in range(1, gz_n)]
    far = [offset for offset in others if offset[2] == 0]
    direct = ITERS - 2

    def begin_sums(i, sums):
        row = jnp.zeros((1, LANES), jnp.float32)
        for n, share in enumerate(sums):
            total = jnp.sum(jnp.sum(share, axis=0, keepdims=True), axis=1, keepdims=True)
            row = jnp.where(lane_row == n, total, row)
        mine[i] = row
        if i >= direct:
            rows_all[i, me] = row
            row_copies(i, mine, rows_all, me, sum_send.at[0], sum_recv.at[i, 0], others)
        else:
            rows_near[i, gz] = row
            row_copies(i, mine, rows_near, gz, sum_send.at[0], sum_recv.at[i, 0], near)

    def forward_sums(i):
        wait_rows(i, rows_near, len(near), sum_recv.at[i, 0])
        row = jnp.sum(rows_near[i], axis=0)
        group = gx * gy_n + gy
        ours[i] = row
        rows_all[i, group] = row
        row_copies(i, ours, rows_all, group, sum_send.at[1], sum_recv.at[i, 1], far)

    def end_sums(i):
        if i >= direct:
            wait_rows(i, rows_all, len(others), sum_recv.at[i, 0])
            row = jnp.sum(rows_all[i], axis=0)
            wait_rows(i, rows_all, len(others), sum_send.at[0])
        else:
            wait_rows(i, rows_all, len(far), sum_recv.at[i, 1])
            row = jnp.sum(rows_all[i, 0 : gx_n * gy_n], axis=0)
            wait_rows(i, rows_near, len(near), sum_send.at[0])
            wait_rows(i, rows_all, len(far), sum_send.at[1])
        return [
            jnp.sum(jnp.where(lane_row == n, row, 0.0), axis=1, keepdims=True) for n in range(2 * SETS)
        ]

    norm, size, alpha, beta = {}, {}, {}, {}

    def scalars(i):
        totals = end_sums(i)
        norm[i], product = totals[:SETS], totals[SETS:]
        if i == 0:
            size[i] = [n / d for n, d in zip(norm[i], product)]
        else:
            ratio = [n / w for n, w in zip(norm[i], norm[i - 1])]
            size[i] = [n / (d - b * n / a) for n, d, b, a in zip(norm[i], product, ratio, size[i - 1])]
            beta[i] = [jnp.broadcast_to(b, (8, LANES)) for b in ratio]
        alpha[i] = [jnp.broadcast_to(a, (8, LANES)) for a in size[i]]

    def advance(i):
        scalars(i)

        def body(x, sums):
            sums = list(sums)
            for s in range(SETS):
                for yb in range(yb_n):
                    at = (s, x, rows_of(yb), slice(None))
                    q = fp[s, x + 1, inner_rows(yb), :]
                    q_image = ft[s, x + 1, inner_rows(yb), :]
                    if i > 0:
                        q = q + beta[i][s] * ss[at]
                        q_image = q_image + beta[i][s] * sa[at]
                    if i + 2 < ITERS:
                        ss[at], sa[at] = q, q_image
                    fresh, fresh_image = (rr, ra) if i % 2 else (rs, rt)
                    old, old_image = (rs, rt) if i % 2 else (rr, ra)
                    r = old[at] - alpha[i][s] * q
                    r_image = old_image[at] - alpha[i][s] * q_image
                    fresh[at], fresh_image[at] = r, r_image
                    square = r * r
                    sums[s] = sums[s] + square
                    sums[SETS + s] = sums[SETS + s] + (r_image * r_image + ww[at] * square)
            return tuple(sums)
        begin_sums(i + 1, sweep(body, (zero,) * (2 * SETS), 0, nx, 4))

        def settle(x, _):
            old, old_image = (rs, rt) if i % 2 else (rr, ra)
            for s in range(SETS):
                for yb in range(yb_n):
                    at = (s, x, rows_of(yb), slice(None))
                    p, p_image = old[at], old_image[at]
                    if i > 0:
                        p = p + beta[i][s] * pp[at]
                        p_image = p_image + beta[i][s] * ap[at]
                    pp[at], ap[at] = p, p_image
                    xx[at] += alpha[i][s] * p
                    ax[at] += alpha[i][s] * p_image
            return _
        sweep(settle, 0, 0, nx, 4)

    no_faces = (zero,) * yb_n

    def sent(ys, s, x, yb, tile, acc):
        keep_rows(ys, s, x, yb, tile)
        acc = list(acc)
        acc[yb] = packed(acc[yb], s, x, tile)
        return tuple(acc)

    def send(kind, parts, acc):
        put_packed(parts[2], acc)
        copies = faces(kind, *parts)
        start(copies)
        return copies

    loads[0].wait()
    face_pass(fp, ysp, zsp)
    loads[2].wait()
    sweep(kappa, 0, 0, nx)
    for load in loads[1:2] + loads[3:]:
        load.wait()
    build(0)
    observe(0, 0, 2)
    pl.semaphore_wait(barrier, len(others))
    p_copies = faces(0, *p_kind)
    start(p_copies)

    def gap():
        build(1)
        observe(1, 0, 2)

    def emit_start(s, x, yb, out, acc):
        ft[s, x + 1, inner_rows(yb), :] = out
        ax[s, x, rows_of(yb), :] = out
        return sent(yst, s, x, yb, out, acc)

    t_copies = send(1, t_kind, apply(fp, p_copies, yrp, zrp, emit_start, no_faces, gap))
    s_copies = faces(2, *s_kind)

    def gap():
        face_pass(fs, yss, zss)
        start(s_copies)

    def emit_residual(s, x, yb, out, acc):
        at = (s, x, rows_of(yb), slice(None))
        r = bb[at] - (out + ww[at] * xx[at])
        rr[at] = r
        fp[s, x + 1, inner_rows(yb), :] = r
        return sent(ysp, s, x, yb, r, acc)

    p_copies = send(0, p_kind, apply(ft, t_copies, yrt, zrt, emit_residual, no_faces, gap))

    def emit_state(s, x, yb, out, carry):
        ast[s, x, rows_of(yb), :] = out
        return carry

    def emit_first(s, x, yb, out, carry):
        at = (s, x, rows_of(yb), slice(None))
        ft[s, x + 1, inner_rows(yb), :] = out
        ra[at] = out
        acc, sums = carry[0], list(carry[1])
        square = rr[at] * rr[at]
        sums[s] = sums[s] + square
        sums[SETS + s] = sums[SETS + s] + (out * out + ww[at] * square)
        return (sent(yst, s, x, yb, out, acc), tuple(sums))

    acc, sums = apply(fp, p_copies, yrp, zrp, emit_first, (no_faces, (zero,) * (2 * SETS)))
    t_copies = send(1, t_kind, acc)
    begin_sums(0, sums)

    def emit_image(s, x, yb, out, acc):
        at = (s, x, rows_of(yb), slice(None))
        w = out + ww[at] * rr[at]
        fp[s, x + 1, inner_rows(yb), :] = w
        return sent(ysp, s, x, yb, w, acc)

    acc = apply(
        ft, t_copies, yrt, zrt, emit_image, no_faces,
        lambda: apply(fs, s_copies, yrs, zrs, emit_state, 0, part=ast),
    )
    p_copies = send(0, p_kind, acc)
    forward_sums(0)

    for i in range(ITERS - 1):
        last = i + 2 == ITERS

        def emit_inner(s, x, yb, out, acc):
            ft[s, x + 1, inner_rows(yb), :] = out
            return acc if last else sent(yst, s, x, yb, out, acc)

        def emit_outer(s, x, yb, out, acc):
            at = (s, x, rows_of(yb), slice(None))
            w = fp[s, x + 1, inner_rows(yb), :]
            z = out + ww[at] * w
            if i > 0:
                z = z + beta[i][s] * zz[at]
            if i + 3 < ITERS:
                zz[at] = z
            w = w - alpha[i][s] * z
            fp[s, x + 1, inner_rows(yb), :] = w
            return sent(ysp, s, x, yb, w, acc)

        acc = apply(fp, p_copies, yrp, zrp, emit_inner, no_faces)
        if last:
            advance(i)
        else:
            t_copies = send(1, t_kind, acc)
            acc = apply(
                ft, t_copies, yrt, zrt, emit_outer, no_faces, functools.partial(advance, i)
            )
            p_copies = send(0, p_kind, acc)
            if i + 1 < direct:
                forward_sums(i + 1)

    i = ITERS - 1
    scalars(i)

    final, final_image = (rr, ra) if (ITERS - 2) % 2 else (rs, rt)

    def finish(x, _):
        for yb in range(yb_n):
            total = zero
            for s in range(SETS):
                at = (s, x, rows_of(yb), slice(None))
                p = final[at] + beta[i][s] * pp[at]
                p_image = final_image[at] + beta[i][s] * ap[at]
                adjoint = xx[at] + alpha[i][s] * p
                image = ax[at] + alpha[i][s] * p_image
                xx[at] = adjoint
                total = total + (adjoint * ast[at] + image * fs[s, x + 1, inner_rows(yb), :])
            kap[x, rows_of(yb), :] = -2.0 * kap[x, rows_of(yb), :] * total
        return _

    stores = []
    share = nx // 4
    for n in range(4):
        sweep(finish, 0, n * share, (n + 1) * share, 2)
        at = pl.ds(n * share, share)
        stores.append(pltpu.make_async_copy(xx.at[:, at], adj_ref.at[:, at], out_sem.at[n, 0]))
        stores.append(pltpu.make_async_copy(kap.at[at], grad_ref.at[at], out_sem.at[n, 1]))
        stores[-2].start()
        stores[-1].start()
    for store in stores:
        store.wait()


def hand_over(gradient, adjoint):
    nx, ny, nz = gradient.shape
    share = nx // 4

    def body(gradient_hbm, adjoint_hbm, gradient_out, adjoint_out, gradient_buf, adjoint_buf, got, put):
        reads, writes = [], []
        for n in range(4):
            at = pl.ds(n * share, share)
            reads += [
                pltpu.make_async_copy(gradient_hbm.at[at], gradient_buf.at[at], got.at[n, 0]),
                pltpu.make_async_copy(adjoint_hbm.at[:, at], adjoint_buf.at[:, at], got.at[n, 1]),
            ]
            writes += [
                pltpu.make_async_copy(gradient_buf.at[at], gradient_out.at[at], put.at[n, 0]),
                pltpu.make_async_copy(adjoint_buf.at[:, at], adjoint_out.at[:, at], put.at[n, 1]),
            ]
        for read in reads:
            read.start()
        for read, write in zip(reads, writes):
            read.wait()
            write.start()
        for write in writes:
            write.wait()

    hbm = pl.BlockSpec(memory_space=pl.ANY)
    return pl.pallas_call(
        body,
        out_shape=(
            jax.ShapeDtypeStruct(gradient.shape, gradient.dtype),
            jax.ShapeDtypeStruct(adjoint.shape, adjoint.dtype),
        ),
        in_specs=[hbm, hbm], out_specs=(hbm, hbm),
        scratch_shapes=[
            pltpu.VMEM(gradient.shape, gradient.dtype), pltpu.VMEM(adjoint.shape, adjoint.dtype),
            pltpu.SemaphoreType.DMA((4, 2)), pltpu.SemaphoreType.DMA((4, 2)),
        ],
        compiler_params=pltpu.CompilerParams(vmem_limit_bytes=60 * 1024 * 1024),
    )(gradient, adjoint)


def on_device(sizes, log_range, state, adjoint_start, obs_index, obs_value):
    nx, ny, nz = log_range.shape
    nobs = obs_index.shape[-1]
    f32 = jnp.float32
    field = pltpu.VMEM((SETS, nx, ny, nz), f32)
    padded = pltpu.VMEM((SETS, nx + 2, ny + 2 * TOP, nz), f32)
    yface = pltpu.VMEM((2, SETS, nx, nz), f32)
    zsent = pltpu.VMEM((ny, LANES), f32)
    zgot = pltpu.VMEM((2, ny, LANES), f32)
    hbm = pl.BlockSpec(memory_space=pl.ANY)
    dma = pltpu.SemaphoreType.DMA
    gradient, adjoint = pl.pallas_call(
        functools.partial(kernel, sizes),
        out_shape=(
            jax.ShapeDtypeStruct((nx, ny, nz), f32),
            jax.ShapeDtypeStruct((SETS, nx, ny, nz), f32),
        ),
        in_specs=[hbm] * 5,
        out_specs=(hbm, hbm),
        scratch_shapes=[
            pltpu.VMEM((nx, ny, nz), f32),
            padded, padded, padded, field, field,
            field, field, field, field, field, field, field, field, field, field, field, field, field,
            yface, yface, yface, zsent, zsent, zsent, yface, yface, yface, zgot, zgot, zgot,
            pltpu.VMEM((6 * LANES, nobs), jnp.bfloat16),
            pltpu.VMEM((256, nobs), jnp.bfloat16),
            pltpu.VMEM((SETS, 1, nobs), jnp.int32),
            pltpu.VMEM((SETS, 1, nobs), f32),
            pltpu.VMEM((ITERS, sizes[0] * sizes[1] * sizes[2], 1, LANES), f32),
            pltpu.VMEM((ITERS, sizes[2], 1, LANES), f32),
            pltpu.VMEM((ITERS, 1, LANES), f32),
            pltpu.VMEM((ITERS, 1, LANES), f32),
            dma((3, 6)), dma((3, 6)), dma((2,)), dma((ITERS, 2)),
            dma((6,)), dma((4, 2)),
        ],
        compiler_params=pltpu.CompilerParams(
            collective_id=0, has_side_effects=True, vmem_limit_bytes=60 * 1024 * 1024
        ),
    )(
        log_range, state, adjoint_start,
        obs_index.reshape(SETS, 1, nobs), obs_value.reshape(SETS, 1, nobs),
    )
    return hand_over(gradient, adjoint)


def solution(mesh):
    sizes = (mesh.shape["gx"], mesh.shape["gy"], mesh.shape["gz"])
    whole, per_set = P("gx", "gy", "gz"), P(None, "gx", "gy", "gz")
    obs = P(None, "gx", "gy", "gz", None)
    return jax.shard_map(
        functools.partial(on_device, sizes), mesh=mesh,
        in_specs=(whole, per_set, per_set, obs, obs), out_specs=(whole, per_set), check_vma=False,
    )
```
